128 devices in a mesh: fsdp: 2 (over core), ep: 64 (over z, y, x).
Axes of the slice: x: 4, y: 4, z: 4, core: 2. Of those that a mesh axis runs over, the one named last changes fastest.
Arguments:
- grad_out: bfloat16 [8192, 1536], P(('fsdp', 'ep'))
- expert_idx: int32 [8192, 6], P(('fsdp', 'ep'))
- slot_pos: int32 [8192, 6], P(('fsdp', 'ep'))
- gates: float32 [8192, 6], P(('fsdp', 'ep'))
- x_disp: bfloat16 [64, 1024, 1536], P('ep', 'fsdp')
- h_gate: bfloat16 [64, 1024, 512], P('ep', 'fsdp')
- h_up: bfloat16 [64, 1024, 512], P('ep', 'fsdp')
- y_disp: bfloat16 [64, 1024, 1536], P('ep', 'fsdp')
- w_gate: bfloat16 [64, 1536, 512], P('ep', 'fsdp')
- w_down: bfloat16 [64, 512, 1536], P('ep', 'fsdp')
- w_up: bfloat16 [64, 1536, 512], P('ep', 'fsdp')
Outputs:
- output 1: bfloat16 [8192, 1536], P(('fsdp', 'ep'))
- output 2: float32 [8192, 6], P(('fsdp', 'ep'))
- output 3: float32 [64, 1536, 512], P('ep', 'fsdp')
- output 4: float32 [64, 512, 1536], P('ep', 'fsdp')
- output 5: float32 [64, 1536, 512], P('ep', 'fsdp')
All inputs are finite; a program needn't handle non-finite values.
Results may differ from the reference program's by a relative error of at most 0.00882546.
Values are sent between devices in bfloat16 or wider.
A program may use at most 1 GiB of HBM per device.

```python
import jax
import jax.numpy as jnp
from jax import lax

D = 1536
F = 512
EXPERTS = 64
TOP = 6
TOK = 64
NDEV = 128
CAP = 8


def route_draw(key):
    key_bias, key_noise, key_hot = jax.random.split(key, 3)
    expert_ids = jnp.arange(EXPERTS, dtype=jnp.int32)
    expert_bias = jax.random.randint(key_bias, (EXPERTS,), 0, 512, dtype=jnp.int32)
    noise_int = jax.random.randint(key_noise, (NDEV, TOK, EXPERTS), 0, 1024, dtype=jnp.int32)
    hot_expert = jax.random.randint(key_hot, (NDEV,), 0, EXPERTS, dtype=jnp.int32)
    forced = (jnp.arange(TOK, dtype=jnp.int32)[None, :, None] <= CAP) & (expert_ids[None, None, :] == hot_expert[:, None, None])
    score_int = (noise_int + expert_bias + jnp.where(forced, 4096, 0)) * EXPERTS + expert_ids
    expert_idx = lax.top_k(score_int, TOP)[1].astype(jnp.int32)

    def block_slots(block_idx):
        flat_ids = block_idx.reshape(-1)
        hit_mask = (flat_ids[:, None] == expert_ids[None, :]).astype(jnp.int32)
        slot_rank = jnp.sum((jnp.cumsum(hit_mask, axis=0) - hit_mask) * hit_mask, axis=1)
        return jnp.where(slot_rank < CAP, slot_rank, -1).reshape(TOK, TOP)

    slot_pos = lax.map(block_slots, expert_idx)
    return expert_idx.reshape(NDEV * TOK, TOP), slot_pos.reshape(NDEV * TOK, TOP).astype(jnp.int32)


def setup_inputs(seed: int = 0) -> dict:
    keys = jax.random.split(jax.random.key(seed), 11)
    expert_idx, slot_pos = route_draw(keys[0])
    rows_all = NDEV * CAP
    grad_out = jax.random.normal(keys[1], (NDEV * TOK, D), jnp.float32).astype(jnp.bfloat16)
    gates = jax.random.uniform(keys[2], (NDEV * TOK, TOP), jnp.float32, 0.2, 1.0)
    x_disp = jax.random.normal(keys[3], (EXPERTS, rows_all, D), jnp.float32).astype(jnp.bfloat16)
    h_gate = jax.random.normal(keys[4], (EXPERTS, rows_all, F), jnp.float32).astype(jnp.bfloat16)
    h_up = jax.random.normal(keys[5], (EXPERTS, rows_all, F), jnp.float32).astype(jnp.bfloat16)
    y_disp = (0.25 * jax.random.normal(keys[6], (EXPERTS, rows_all, D), jnp.float32)).astype(jnp.bfloat16)
    w_gate = (jax.random.normal(keys[7], (EXPERTS, D, F), jnp.float32) * D ** -0.5).astype(jnp.bfloat16)
    w_down = (jax.random.normal(keys[8], (EXPERTS, F, D), jnp.float32) * F ** -0.5).astype(jnp.bfloat16)
    w_up = (jax.random.normal(keys[9], (EXPERTS, D, F), jnp.float32) * D ** -0.5).astype(jnp.bfloat16)
    return {'grad_out': grad_out, 'expert_idx': expert_idx, 'slot_pos': slot_pos, 'gates': gates, 'x_disp': x_disp, 'h_gate': h_gate, 'h_up': h_up, 'y_disp': y_disp, 'w_gate': w_gate, 'w_down': w_down, 'w_up': w_up}


def expert_backward(operands):
    dy_rows, gate_rows, x_rows, pre_gate, pre_up, y_rows, w_gate, w_down, w_up = operands
    g_rows = (dy_rows.astype(jnp.float32) * gate_rows[:, None]).astype(jnp.bfloat16)
    gate_pre = pre_gate.astype(jnp.float32)
    up_pre = pre_up.astype(jnp.float32)
    sigmoid_gate = jax.nn.sigmoid(gate_pre)
    silu_gate = gate_pre * sigmoid_gate
    act_rows = (silu_gate * up_pre).astype(jnp.bfloat16)
    d_act = jnp.dot(g_rows, w_down.T, preferred_element_type=jnp.float32)
    dh_gate = (d_act * up_pre * sigmoid_gate * (1.0 + gate_pre * (1.0 - sigmoid_gate))).astype(jnp.bfloat16)
    dh_up = (d_act * silu_gate).astype(jnp.bfloat16)
    dx_rows = (jnp.dot(dh_gate, w_gate.T, preferred_element_type=jnp.float32) + jnp.dot(dh_up, w_up.T, preferred_element_type=jnp.float32)).astype(jnp.bfloat16)
    dgate_rows = jnp.sum(dy_rows.astype(jnp.float32) * y_rows.astype(jnp.float32), axis=1)
    dw_gate = jnp.dot(x_rows.T, dh_gate, preferred_element_type=jnp.float32)
    dw_down = jnp.dot(act_rows.T, g_rows, preferred_element_type=jnp.float32)
    dw_up = jnp.dot(x_rows.T, dh_up, preferred_element_type=jnp.float32)
    return dx_rows, dgate_rows, dw_gate, dw_down, dw_up


def reference(grad_out, expert_idx, slot_pos, gates, x_disp, h_gate, h_up, y_disp, w_gate, w_down, w_up):
    rows_all = NDEV * CAP
    choices = NDEV * TOK * TOP
    block_ids = jnp.arange(NDEV * TOK, dtype=jnp.int32)[:, None] // TOK
    dest_row = jnp.where(slot_pos >= 0, expert_idx * rows_all + block_ids * CAP + slot_pos, EXPERTS * rows_all).reshape(-1)
    src_choice = jnp.full((EXPERTS * rows_all,), choices, jnp.int32).at[dest_row].set(jnp.arange(choices, dtype=jnp.int32), mode='drop')
    dy_rows = jnp.take(grad_out, src_choice // TOP, axis=0, mode='fill', fill_value=0).reshape(EXPERTS, rows_all, D)
    gate_rows = jnp.take(gates.reshape(-1), src_choice, mode='fill', fill_value=0).reshape(EXPERTS, rows_all)
    dx_rows, dgate_rows, dw_gate, dw_down, dw_up = lax.map(expert_backward, (dy_rows, gate_rows, x_disp, h_gate, h_up, y_disp, w_gate, w_down, w_up))
    picked = jnp.take(dx_rows.reshape(EXPERTS * rows_all, D), dest_row, axis=0, mode='fill', fill_value=0).reshape(NDEV * TOK, TOP, D)
    grad_x = jnp.sum(picked.astype(jnp.float32), axis=1).astype(jnp.bfloat16)
    grad_gates = jnp.take(dgate_rows.reshape(-1), dest_row, mode='fill', fill_value=0).reshape(NDEV * TOK, TOP)
    return grad_x, grad_gates, dw_gate, dw_down, dw_up
```

```python
import functools

import jax
import jax.numpy as jnp
from jax import lax
from jax.experimental import pallas as pl
from jax.experimental.pallas import tpu as pltpu
from jax.sharding import PartitionSpec as P

MESH = pl.DeviceIdType.MESH
F32 = jnp.float32
BF16 = jnp.bfloat16
PLANES = 4
PLANE_ORDER = (2, 3, 1, 0)
NT = (((1,), (1,)), ((), ()))
TN = (((0,), (0,)), ((), ()))


def layer_kernel(cfg, go, eidx, slot, gates, x_in, hg_in, hu_in, y_in, wg_in, wd_in, wu_in,
                 gx, gg, dwg_out, dwd_out, dwu_out,
                 send, recv, gsend, grecv, dxs, dxr, vs, vr,
                 xv, yv, hgv, huv, wgu, wd, onehot, gv, av, dhv,
                 pg, pd, pu, rg, rd, ru, og, od, ou,
                 load_sem, wsend_sem, wrecv_sem, fsend_sem, frecv_sem, gsend_sem, grecv_sem,
                 bsend_sem, brecv_sem, vsend_sem, vrecv_sem, psend_sem, precv_sem, out_sem):
    ep_n, top, tok_n, width, hidden, cap, ysz, xsz = cfg
    plane = ep_n // PLANES
    lanes = plane * cap
    rows_chunk = plane * cap
    half_d, half_f = width // 2, hidden // 2
    q = lax.axis_index('fsdp')
    me = lax.axis_index('ep')
    other = 1 - q
    my_plane = me // plane
    my_in = lax.rem(me, plane)

    def peer_in(o):
        oy, ox = o // xsz, lax.rem(o, xsz)
        return lax.rem(my_in // xsz + oy, ysz) * xsz + lax.rem(my_in + ox, xsz)

    barrier = pltpu.get_barrier_semaphore()

    def announce(o, c):
        pl.semaphore_signal(barrier, inc=1, device_id=(q, lax.rem(me + o, ep_n)), device_id_type=MESH)
        return c

    lax.fori_loop(1, ep_n, announce, 0)
    pl.semaphore_signal(barrier, inc=1, device_id=(other, me), device_id_type=MESH)

    loads = [
        pltpu.make_async_copy(wd_in, wd.at[pl.ds(q * half_f, half_f)], load_sem.at[0]),
        pltpu.make_async_copy(wg_in, wgu.at[pl.ds(q * half_d, half_d), pl.ds(0, hidden)], load_sem.at[1]),
        pltpu.make_async_copy(wu_in, wgu.at[pl.ds(q * half_d, half_d), pl.ds(hidden, hidden)], load_sem.at[2]),
        pltpu.make_async_copy(hg_in, hgv, load_sem.at[3]),
        pltpu.make_async_copy(hu_in, huv, load_sem.at[4]),
        pltpu.make_async_copy(y_in, yv, load_sem.at[5]),
        pltpu.make_async_copy(x_in, xv, load_sem.at[6]),
    ]
    for cp in loads:
        cp.start()

    dest = jnp.where(slot[...] >= 0, eidx[...] * cap + slot[...], ep_n * cap)
    lane_t = lax.broadcasted_iota(jnp.int32, (tok_n, lanes), 1)
    for k in range(PLANES):
        hot = jnp.zeros((tok_n, lanes), F32)
        gate = jnp.zeros((tok_n, lanes), F32)
        for j in range(top):
            hit = lane_t == dest[:, j:j + 1] - k * lanes
            hot = jnp.where(hit, 1.0, hot)
            gate = jnp.where(hit, gates[:, j:j + 1], gate)
        hot = hot.astype(BF16)
        onehot[k] = hot
        gsend[k] = jnp.sum(gate, axis=0, keepdims=True)
        picked = lax.dot_general(hot, go[...], TN, preferred_element_type=F32)
        send[pl.ds(k * plane, plane)] = picked.reshape(plane, cap, width).astype(BF16)

    pl.semaphore_wait(barrier, ep_n)

    def partner_copy(src, dst, i, ssem, rsem):
        return pltpu.make_async_remote_copy(src_ref=src, dst_ref=dst, send_sem=ssem.at[i], recv_sem=rsem.at[i],
                                            device_id=(other, me), device_id_type=MESH)

    wcopies = [
        partner_copy(wd_in, wd.at[pl.ds(q * half_f, half_f)], 0, wsend_sem, wrecv_sem),
        partner_copy(wg_in, wgu.at[pl.ds(q * half_d, half_d), pl.ds(0, hidden)], 1, wsend_sem, wrecv_sem),
        partner_copy(wu_in, wgu.at[pl.ds(q * half_d, half_d), pl.ds(hidden, hidden)], 2, wsend_sem, wrecv_sem),
    ]
    for cp in wcopies:
        cp.start()

    def row_copy(src, dst, idx, ssem, rsem):
        return pltpu.make_async_remote_copy(src_ref=src.at[idx], dst_ref=dst.at[me], send_sem=ssem,
                                            recv_sem=rsem.at[my_plane], device_id=(q, idx), device_id_type=MESH)

    def gate_copy(idx):
        return pltpu.make_async_remote_copy(src_ref=gsend.at[idx // plane], dst_ref=grecv.at[me], send_sem=gsend_sem,
                                            recv_sem=grecv_sem.at[my_plane], device_id=(q, idx), device_id_type=MESH)

    for ci, dz in enumerate(PLANE_ORDER):
        to_plane = lax.rem(my_plane + PLANES - dz, PLANES)

        def send_one(o, c, to_plane=to_plane):
            idx = to_plane * plane + peer_in(o)
            gate_copy(idx).start()
            row_copy(send, recv, idx, fsend_sem, frecv_sem).start()
            return c

        lax.fori_loop(1 if dz == 0 else 0, plane, send_one, 0)
    recv[me] = send[me]
    grecv[me] = gsend[my_plane]

    def wait_bytes(buf, n, sem):
        part = buf.at[pl.ds(0, n)]
        pltpu.make_async_copy(part, part, sem).wait()

    def wait_chunk(ci, buf, sem):
        @pl.when(ci < PLANES - 1)
        def _():
            wait_bytes(buf, plane, sem)

        @pl.when(ci == PLANES - 1)
        def _():
            wait_bytes(buf, plane - 1, sem)

    for i in (0, 1, 2):
        loads[i].wait()
        wcopies[i].wait()
    for i in (3, 4, 5):
        loads[i].wait()

    lane_c = lax.broadcasted_iota(jnp.int32, (plane, cap, lanes), 2)
    sub_c = lax.broadcasted_iota(jnp.int32, (plane, cap, lanes), 1)
    mine = lane_c == my_in * cap + sub_c

    def plane_at(ci):
        n = PLANES - 1 - ci
        dz = n + (n // 2) * (5 - 2 * n)
        return lax.rem(my_plane + dz, PLANES)

    def chunk(ci, c):
        zp = plane_at(ci)
        wait_chunk(ci, recv, frecv_sem.at[zp])
        wait_chunk(ci, grecv, grecv_sem.at[zp])
        rows = pl.ds(zp * rows_chunk, rows_chunk)
        blocks = pl.ds(zp * plane, plane)
        dy = recv[blocks].astype(F32).reshape(rows_chunk, width)
        gate3 = jnp.where(mine, jnp.broadcast_to(grecv[blocks], (plane, cap, lanes)), 0.0)
        gate = jnp.sum(gate3, axis=2, keepdims=True).reshape(rows_chunk, 1)
        g = (dy * gate).astype(BF16)
        gv[rows] = g
        val = jnp.sum(dy * yv[rows].astype(F32), axis=1, keepdims=True).reshape(plane, cap, 1)
        vs[blocks] = jnp.sum(jnp.where(mine, val, 0.0), axis=1, keepdims=True)
        da = lax.dot_general(g, wd[...], NT, preferred_element_type=F32)
        h1 = hgv[rows].astype(F32)
        h3 = huv[rows].astype(F32)
        sg = jax.nn.sigmoid(h1)
        silu = h1 * sg
        av[rows] = jnp.where(gate > 0.0, silu * h3, 0.0).astype(BF16)
        dhv[rows, pl.ds(0, hidden)] = (da * h3 * sg * (1.0 + h1 * (1.0 - sg))).astype(BF16)
        dhv[rows, pl.ds(hidden, hidden)] = (da * silu).astype(BF16)
        dx = lax.dot_general(dhv[rows], wgu[...], NT, preferred_element_type=F32)
        dxs[blocks] = dx.reshape(plane, cap, width).astype(BF16)

        def back_one(o, cc):
            idx = zp * plane + peer_in(o)

            @pl.when(jnp.logical_or(ci < PLANES - 1, o > 0))
            def _():
                row_copy(dxs, dxr, idx, bsend_sem, brecv_sem).start()
                row_copy(vs, vr, idx, vsend_sem, vrecv_sem).start()

            return cc

        lax.fori_loop(0, plane, back_one, 0)
        return c

    lax.fori_loop(0, PLANES, chunk, 0)
    dxr[me] = dxs[me]
    vr[me] = vs[me]

    loads[6].wait()

    def in_grads(base, to_g, to_u):
        tile = 256 if half_d % 256 == 0 else half_d

        def step(i, c):
            cols = pl.ds(pl.multiple_of(base + i * tile, tile), tile)
            r = lax.dot_general(xv[:, cols], dhv[...], TN, preferred_element_type=F32)
            to_g[pl.ds(i * tile, tile)] = r[:, :hidden]
            to_u[pl.ds(i * tile, tile)] = r[:, hidden:]
            return c

        lax.fori_loop(0, half_d // tile, step, 0)

    def out_grads(base, to_d):
        cols = pl.ds(pl.multiple_of(base, half_f), half_f)
        to_d[...] = lax.dot_general(av[:, cols], gv[...], TN, preferred_element_type=F32)

    in_grads(other * half_d, pg, pu)
    pcopies = [partner_copy(pg, rg, 0, psend_sem, precv_sem), partner_copy(pu, ru, 1, psend_sem, precv_sem)]
    pcopies[0].start()
    pcopies[1].start()
    out_grads(other * half_f, pd)
    pcopies.append(partner_copy(pd, rd, 2, psend_sem, precv_sem))
    pcopies[2].start()
    in_grads(q * half_d, og, ou)
    out_grads(q * half_f, od)
    outs = []
    for i, (mine_ref, got, out) in enumerate(((og, rg, dwg_out), (ou, ru, dwu_out), (od, rd, dwd_out))):
        pcopies[i].wait()
        mine_ref[...] += got[...]
        cp = pltpu.make_async_copy(mine_ref, out, out_sem.at[i])
        cp.start()
        outs.append(cp)

    acc = jnp.zeros((tok_n, width), F32)
    vals = [jnp.zeros((tok_n, lanes), F32) for _ in range(top)]
    for ci, dz in enumerate(PLANE_ORDER):
        zp = lax.rem(my_plane + PLANES - dz, PLANES)
        n = plane - 1 if dz == 0 else plane
        wait_bytes(dxr, n, brecv_sem.at[zp])
        wait_bytes(vr, n, vrecv_sem.at[zp])
        blocks = pl.ds(zp * plane, plane)
        part = dxr[blocks].astype(F32).reshape(rows_chunk, width).astype(BF16)
        acc = acc + jnp.dot(onehot[zp], part, preferred_element_type=F32)
        back = jnp.sum(vr[blocks], axis=0)
        for j in range(top):
            hit = lane_t == dest[:, j:j + 1] - zp * lanes
            vals[j] = jnp.where(hit, back, vals[j])
    gx[...] = acc.astype(BF16)
    lane_k = lax.broadcasted_iota(jnp.int32, (tok_n, top), 1)
    gates_out = jnp.zeros((tok_n, top), F32)
    for j in range(top):
        gates_out = jnp.where(lane_k == j, jnp.sum(vals[j], axis=1, keepdims=True), gates_out)
    gg[...] = gates_out

    def wait_sent(buf, n, sem):
        part = buf.at[pl.ds(0, n)]
        pltpu.make_async_copy(part, part, sem).wait()

    wait_sent(send, ep_n - 1, fsend_sem)
    wait_sent(grecv, ep_n - 1, gsend_sem)
    wait_sent(dxs, ep_n - 1, bsend_sem)
    wait_sent(vs, ep_n - 1, vsend_sem)
    for cp in outs:
        cp.wait()


def solution(mesh):
    ep_n = mesh.shape['ep']
    tok_spec = P(('fsdp', 'ep'), None)
    row_spec = P('ep', 'fsdp', None)

    def local_backward(grad_out, expert_idx, slot_pos, gates, x_disp, h_gate, h_up, y_disp, w_gate, w_down, w_up):
        tok_n, top = expert_idx.shape
        _, rows, width = x_disp.shape
        hidden = h_gate.shape[2]
        cap = rows // ep_n
        plane = ep_n // PLANES
        ysz = 4 if plane == 16 else 2
        xsz = plane // ysz
        lanes = plane * cap
        half_d, half_f = width // 2, hidden // 2
        cfg = (ep_n, top, tok_n, width, hidden, cap, ysz, xsz)
        vmem = pl.BlockSpec(memory_space=pltpu.VMEM)
        hbm = pl.BlockSpec(memory_space=pl.ANY)
        dma = pltpu.SemaphoreType.DMA
        rows_buf = pltpu.VMEM((ep_n, cap, width), BF16)
        gate_buf = pltpu.VMEM((ep_n, 1, lanes), F32)
        in_part = pltpu.VMEM((half_d, hidden), F32)
        out_part = pltpu.VMEM((half_f, width), F32)
        outs = pl.pallas_call(
            functools.partial(layer_kernel, cfg),
            out_shape=[
                jax.ShapeDtypeStruct((tok_n, width), BF16),
                jax.ShapeDtypeStruct((tok_n, top), F32),
                jax.ShapeDtypeStruct((half_d, hidden), F32),
                jax.ShapeDtypeStruct((half_f, width), F32),
                jax.ShapeDtypeStruct((half_d, hidden), F32),
            ],
            in_specs=[vmem] * 4 + [hbm] * 7,
            out_specs=[vmem] * 2 + [hbm] * 3,
            scratch_shapes=[
                rows_buf, rows_buf, pltpu.VMEM((PLANES, 1, lanes), F32), gate_buf, rows_buf, rows_buf, gate_buf, gate_buf,
                pltpu.VMEM((rows, width), BF16), pltpu.VMEM((rows, width), BF16),
                pltpu.VMEM((rows, hidden), BF16), pltpu.VMEM((rows, hidden), BF16),
                pltpu.VMEM((width, 2 * hidden), BF16), pltpu.VMEM((hidden, width), BF16),
                pltpu.VMEM((PLANES, tok_n, lanes), BF16),
                pltpu.VMEM((rows, width), BF16), pltpu.VMEM((rows, hidden), BF16), pltpu.VMEM((rows, 2 * hidden), BF16),
                in_part, out_part, in_part, in_part, out_part, in_part, in_part, out_part, in_part,
                dma((7,)), dma((3,)), dma((3,)), dma, dma((PLANES,)), dma, dma((PLANES,)),
                dma, dma((PLANES,)), dma, dma((PLANES,)), dma((3,)), dma((3,)), dma((3,)),
            ],
            compiler_params=pltpu.CompilerParams(collective_id=0, has_side_effects=True, vmem_limit_bytes=60 * 1024 * 1024),
            name='layer',
        )(grad_out, expert_idx, slot_pos, gates, x_disp[0], h_gate[0], h_up[0], y_disp[0], w_gate[0], w_down[0], w_up[0])
        gx, gg, dwg, dwd, dwu = outs
        return gx, gg, dwg[None], dwd[None], dwu[None]

    return jax.shard_map(local_backward, mesh=mesh, in_specs=(tok_spec, tok_spec, tok_spec, tok_spec, row_spec, row_spec, row_spec, row_spec, row_spec, row_spec, row_spec), out_specs=(tok_spec, tok_spec, row_spec, row_spec, row_spec), check_vma=False)
```

```python
import functools

import jax
import jax.numpy as jnp
from jax import lax
from jax.experimental import pallas as pl
from jax.experimental.pallas import tpu as pltpu
from jax.sharding import PartitionSpec as P

MESH = pl.DeviceIdType.MESH
F32 = jnp.float32
BF16 = jnp.bfloat16
PLANES = 4
PLANE_ORDER = (1, 3, 2, 0)
NT = (((1,), (1,)), ((), ()))
TN = (((0,), (0,)), ((), ()))


def layer_kernel(cfg, go_in, eidx_in, slot_in, gates_in, x_in, hg_in, hu_in, y_in, wg_in, wd_in, wu_in,
                 gx, gg, og, od, ou,
                 go, eidx, slot, gates, send, recv, gsend, grecv, dxs, dxr, vs, vr,
                 xv, yv, hgv, huv, wgu, wd, onehot, gv, av, dhv,
                 pg, pd, pu, rg, rd, ru,
                 load_sem, wsend_sem, wrecv_sem, fsend_sem, frecv_sem, gsend_sem, grecv_sem,
                 bsend_sem, brecv_sem, vsend_sem, vrecv_sem, psend_sem, precv_sem):
    ep_n, top, tok_n, width, hidden, cap, ysz, xsz = cfg
    plane = ep_n // PLANES
    lanes = plane * cap
    rows_chunk = plane * cap
    half_d, half_f = width // 2, hidden // 2
    q = lax.axis_index('fsdp')
    me = lax.axis_index('ep')
    other = 1 - q
    my_plane = me // plane
    my_in = lax.rem(me, plane)

    def peer_in(o):
        half, i = o // (plane // 2), lax.rem(o, plane // 2)
        oy = i // (xsz // 2)
        ox = 2 * lax.rem(i, xsz // 2) + lax.rem(oy + half, 2)
        return lax.rem(my_in // xsz + oy, ysz) * xsz + lax.rem(my_in + ox, xsz)

    barrier = pltpu.get_barrier_semaphore()

    def announce(o, c):
        pl.semaphore_signal(barrier, inc=1, device_id=(q, lax.rem(me + o, ep_n)), device_id_type=MESH)
        return c

    lax.fori_loop(1, ep_n, announce, 0)
    pl.semaphore_signal(barrier, inc=1, device_id=(other, me), device_id_type=MESH)

    small = [
        pltpu.make_async_copy(src, dst, load_sem.at[7 + i])
        for i, (src, dst) in enumerate(((eidx_in, eidx), (slot_in, slot), (gates_in, gates), (go_in, go)))
    ]
    for cp in small:
        cp.start()
    loads = [
        pltpu.make_async_copy(wd_in, wd.at[pl.ds(q * half_f, half_f)], load_sem.at[0]),
        pltpu.make_async_copy(wg_in, wgu.at[pl.ds(q * half_d, half_d), pl.ds(0, hidden)], load_sem.at[1]),
        pltpu.make_async_copy(wu_in, wgu.at[pl.ds(q * half_d, half_d), pl.ds(hidden, hidden)], load_sem.at[2]),
        pltpu.make_async_copy(hg_in, hgv, load_sem.at[3]),
        pltpu.make_async_copy(hu_in, huv, load_sem.at[4]),
        pltpu.make_async_copy(y_in, yv, load_sem.at[5]),
        pltpu.make_async_copy(x_in, xv, load_sem.at[6]),
    ]
    for cp in loads:
        cp.start()

    for cp in small:
        cp.wait()
    dest = jnp.where(slot[...] >= 0, eidx[...] * cap + slot[...], ep_n * cap)
    slot_s = lax.broadcasted_iota(jnp.int32, (lanes, tok_n), 0)
    diag = lax.broadcasted_iota(jnp.int32, (lanes, lanes), 0) == lax.broadcasted_iota(jnp.int32, (lanes, lanes), 1)
    for k in range(PLANES):
        hot = jnp.zeros((lanes, tok_n), F32)
        gate = jnp.zeros((lanes, tok_n), F32)
        for j in range(top):
            hit = slot_s == dest[j:j + 1, :] - k * lanes
            hot = jnp.where(hit, 1.0, hot)
            gate = jnp.where(hit, gates[j:j + 1, :], gate)
        hot = hot.astype(BF16)
        onehot[k] = hot
        gate_col = jnp.sum(gate, axis=1, keepdims=True)
        gsend[k] = jnp.sum(jnp.where(diag, gate_col, 0.0), axis=0, keepdims=True)
        picked = jnp.dot(hot, go[...], preferred_element_type=F32)
        send[pl.ds(k * plane, plane)] = picked.reshape(plane, cap, width).astype(BF16)

    pl.semaphore_wait(barrier, ep_n)

    def partner_copy(src, dst, i, ssem, rsem):
        return pltpu.make_async_remote_copy(src_ref=src, dst_ref=dst, send_sem=ssem.at[i], recv_sem=rsem.at[i],
                                            device_id=(other, me), device_id_type=MESH)

    wcopies = [
        partner_copy(wd_in, wd.at[pl.ds(q * half_f, half_f)], 0, wsend_sem, wrecv_sem),
        partner_copy(wg_in, wgu.at[pl.ds(q * half_d, half_d), pl.ds(0, hidden)], 1, wsend_sem, wrecv_sem),
        partner_copy(wu_in, wgu.at[pl.ds(q * half_d, half_d), pl.ds(hidden, hidden)], 2, wsend_sem, wrecv_sem),
    ]
    for cp in wcopies:
        cp.start()

    def row_copy(src, dst, idx, ssem, rsem):
        return pltpu.make_async_remote_copy(src_ref=src.at[idx], dst_ref=dst.at[me], send_sem=ssem,
                                            recv_sem=rsem.at[my_plane], device_id=(q, idx), device_id_type=MESH)

    def gate_copy(idx):
        return pltpu.make_async_remote_copy(src_ref=gsend.at[idx // plane], dst_ref=grecv.at[me], send_sem=gsend_sem,
                                            recv_sem=grecv_sem.at[my_plane], device_id=(q, idx), device_id_type=MESH)

    def wait_bytes(buf, n, sem):
        part = buf.at[pl.ds(0, n)]
        pltpu.make_async_copy(part, part, sem).wait()

    def send_part(part, lo, hi, skip_own):
        first, second = PLANE_ORDER[2 * (part // 2)], PLANE_ORDER[2 * (part // 2) + 1]

        def send_one(o, c):
            for dz in (first, second):
                idx = lax.rem(my_plane + PLANES - dz, PLANES) * plane + peer_in(o)

                def go_now():
                    gate_copy(idx).start()
                    row_copy(send, recv, idx, fsend_sem.at[part], frecv_sem).start()

                if dz == 0 and skip_own:
                    pl.when(o > 0)(go_now)
                else:
                    go_now()
            return c

        lax.fori_loop(lo, hi, send_one, 0)

    half_n = plane // 2
    send_part(0, 0, half_n, False)
    send_part(1, half_n, plane, False)
    recv[me] = send[me]
    grecv[me] = gsend[my_plane]
    wait_bytes(send, plane, fsend_sem.at[0])
    send_part(2, 0, half_n, True)
    wait_bytes(send, plane, fsend_sem.at[1])
    send_part(3, half_n, plane, False)

    def wait_chunk(ci, buf, sem):
        @pl.when(ci < PLANES - 1)
        def _():
            wait_bytes(buf, plane, sem)

        @pl.when(ci == PLANES - 1)
        def _():
            wait_bytes(buf, plane - 1, sem)

    for i in (0, 1, 2):
        loads[i].wait()
        wcopies[i].wait()
    for i in (3, 4, 5):
        loads[i].wait()

    lane_c = lax.broadcasted_iota(jnp.int32, (plane, cap, lanes), 2)
    sub_c = lax.broadcasted_iota(jnp.int32, (plane, cap, lanes), 1)
    mine = lane_c == my_in * cap + sub_c

    def plane_at(ci):
        n = lax.rem(ci + 1, PLANES)
        dz = n + (n // 2) * (5 - 2 * n)
        return lax.rem(my_plane + dz, PLANES)

    def chunk(ci, c):
        zp = plane_at(ci)
        wait_chunk(ci, recv, frecv_sem.at[zp])
        wait_chunk(ci, grecv, grecv_sem.at[zp])
        rows = pl.ds(zp * rows_chunk, rows_chunk)
        blocks = pl.ds(zp * plane, plane)
        dy = recv[blocks].astype(F32).reshape(rows_chunk, width)
        gate3 = jnp.where(mine, jnp.broadcast_to(grecv[blocks], (plane, cap, lanes)), 0.0)
        gate = jnp.sum(gate3, axis=2, keepdims=True).reshape(rows_chunk, 1)
        g = (dy * gate).astype(BF16)
        gv[rows] = g
        val = jnp.sum(dy * yv[rows].astype(F32), axis=1, keepdims=True).reshape(plane, cap, 1)
        vs[blocks] = jnp.sum(jnp.where(mine, val, 0.0), axis=1, keepdims=True)
        da = lax.dot_general(g, wd[...], NT, preferred_element_type=F32)
        h1 = hgv[rows].astype(F32)
        h3 = huv[rows].astype(F32)
        sg = jax.nn.sigmoid(h1)
        silu = h1 * sg
        av[rows] = jnp.where(gate > 0.0, silu * h3, 0.0).astype(BF16)
        dhv[rows, pl.ds(0, hidden)] = (da * h3 * sg * (1.0 + h1 * (1.0 - sg))).astype(BF16)
        dhv[rows, pl.ds(hidden, hidden)] = (da * silu).astype(BF16)
        dx = lax.dot_general(dhv[rows], wgu[...], NT, preferred_element_type=F32)
        dxs[blocks] = dx.reshape(plane, cap, width).astype(BF16)

        def back_one(o, cc):
            idx = zp * plane + peer_in(o)

            @pl.when(jnp.logical_or(ci < PLANES - 1, o > 0))
            def _():
                row_copy(dxs, dxr, idx, bsend_sem, brecv_sem).start()
                row_copy(vs, vr, idx, vsend_sem, vrecv_sem).start()

            return cc

        lax.fori_loop(0, plane, back_one, 0)
        return c

    lax.fori_loop(0, PLANES, chunk, 0)
    dxr[me] = dxs[me]
    vr[me] = vs[me]

    loads[6].wait()

    def in_grads(base, to_g, to_u):
        tile = 256 if half_d % 256 == 0 else half_d

        def step(i, c):
            cols = pl.ds(pl.multiple_of(base + i * tile, tile), tile)
            r = lax.dot_general(xv[:, cols], dhv[...], TN, preferred_element_type=F32)
            to_g[pl.ds(i * tile, tile)] = r[:, :hidden]
            to_u[pl.ds(i * tile, tile)] = r[:, hidden:]
            return c

        lax.fori_loop(0, half_d // tile, step, 0)

    def out_grads(base, to_d):
        cols = pl.ds(pl.multiple_of(base, half_f), half_f)
        to_d[...] = lax.dot_general(av[:, cols], gv[...], TN, preferred_element_type=F32)

    in_grads(other * half_d, pg, pu)
    pcopies = [partner_copy(pg, rg, 0, psend_sem, precv_sem), partner_copy(pu, ru, 1, psend_sem, precv_sem)]
    pcopies[0].start()
    pcopies[1].start()
    out_grads(other * half_f, pd)
    pcopies.append(partner_copy(pd, rd, 2, psend_sem, precv_sem))
    pcopies[2].start()
    in_grads(q * half_d, og, ou)
    out_grads(q * half_f, od)
    for i, (mine_ref, got) in enumerate(((og, rg), (ou, ru), (od, rd))):
        pcopies[i].wait()
        mine_ref[...] += got[...]

    acc = jnp.zeros((tok_n, width), F32)
    vals = [jnp.zeros((lanes, tok_n), F32) for _ in range(top)]
    for ci, dz in enumerate(PLANE_ORDER):
        zp = lax.rem(my_plane + PLANES - dz, PLANES)
        n = plane - 1 if dz == 0 else plane
        wait_bytes(dxr, n, brecv_sem.at[zp])
        wait_bytes(vr, n, vrecv_sem.at[zp])
        blocks = pl.ds(zp * plane, plane)
        part = dxr[blocks].astype(F32).reshape(rows_chunk, width).astype(BF16)
        acc = acc + lax.dot_general(onehot[zp], part, TN, preferred_element_type=F32)
        back = jnp.sum(jnp.where(diag, jnp.sum(vr[blocks], axis=0), 0.0), axis=1, keepdims=True)
        for j in range(top):
            hit = slot_s == dest[j:j + 1, :] - zp * lanes
            vals[j] = jnp.where(hit, back, vals[j])
    gx[...] = acc.astype(BF16)
    for j in range(top):
        gg[j:j + 1, :] = jnp.sum(vals[j], axis=0, keepdims=True)

    wait_bytes(send, plane - 1, fsend_sem.at[2])
    wait_bytes(send, plane, fsend_sem.at[3])
    wait_bytes(grecv, ep_n - 1, gsend_sem)
    wait_bytes(dxs, ep_n - 1, bsend_sem)
    wait_bytes(vs, ep_n - 1, vsend_sem)


def write_kernel(*refs):
    n = len(refs) // 2
    sem = refs[-1]
    copies = [pltpu.make_async_copy(refs[i], refs[n + i], sem.at[i]) for i in range(n)]
    for cp in copies:
        cp.start()
    for cp in copies:
        cp.wait()


def solution(mesh):
    ep_n = mesh.shape['ep']
    tok_spec = P(('fsdp', 'ep'), None)
    row_spec = P('ep', 'fsdp', None)

    def local_backward(grad_out, expert_idx, slot_pos, gates, x_disp, h_gate, h_up, y_disp, w_gate, w_down, w_up):
        tok_n, top = expert_idx.shape
        _, rows, width = x_disp.shape
        hidden = h_gate.shape[2]
        cap = rows // ep_n
        plane = ep_n // PLANES
        ysz = 4 if plane == 16 else 2
        xsz = plane // ysz
        lanes = plane * cap
        half_d, half_f = width // 2, hidden // 2
        cfg = (ep_n, top, tok_n, width, hidden, cap, ysz, xsz)
        vmem = pl.BlockSpec(memory_space=pltpu.VMEM)
        hbm = pl.BlockSpec(memory_space=pl.ANY)
        dma = pltpu.SemaphoreType.DMA
        rows_buf = pltpu.VMEM((ep_n, cap, width), BF16)
        gate_buf = pltpu.VMEM((ep_n, 1, lanes), F32)
        in_part = pltpu.VMEM((half_d, hidden), F32)
        out_part = pltpu.VMEM((half_f, width), F32)
        results = [
            jax.ShapeDtypeStruct((tok_n, width), BF16),
            jax.ShapeDtypeStruct((top, tok_n), F32),
            jax.ShapeDtypeStruct((half_d, hidden), F32),
            jax.ShapeDtypeStruct((half_f, width), F32),
            jax.ShapeDtypeStruct((half_d, hidden), F32),
        ]
        outs = pl.pallas_call(
            functools.partial(layer_kernel, cfg),
            out_shape=results,
            in_specs=[hbm] * 11,
            out_specs=[vmem] * 5,
            scratch_shapes=[
                pltpu.VMEM((tok_n, width), BF16), pltpu.VMEM((top, tok_n), jnp.int32), pltpu.VMEM((top, tok_n), jnp.int32),
                pltpu.VMEM((top, tok_n), F32), rows_buf, rows_buf, pltpu.VMEM((PLANES, 1, lanes), F32), gate_buf, rows_buf, rows_buf, gate_buf, gate_buf,
                pltpu.VMEM((rows, width), BF16), pltpu.VMEM((rows, width), BF16),
                pltpu.VMEM((rows, hidden), BF16), pltpu.VMEM((rows, hidden), BF16),
                pltpu.VMEM((width, 2 * hidden), BF16), pltpu.VMEM((hidden, width), BF16),
                pltpu.VMEM((PLANES, lanes, tok_n), BF16),
                pltpu.VMEM((rows, width), BF16), pltpu.VMEM((rows, hidden), BF16), pltpu.VMEM((rows, 2 * hidden), BF16),
                in_part, out_part, in_part, in_part, out_part, in_part,
                dma((11,)), dma((3,)), dma((3,)), dma((4,)), dma((PLANES,)), dma, dma((PLANES,)),
                dma, dma((PLANES,)), dma, dma((PLANES,)), dma((3,)), dma((3,)),
            ],
            compiler_params=pltpu.CompilerParams(collective_id=0, has_side_effects=True, vmem_limit_bytes=44 * 1024 * 1024),
            name='layer',
        )(grad_out, expert_idx.T, slot_pos.T, gates.T, x_disp[0], h_gate[0], h_up[0], y_disp[0], w_gate[0], w_down[0], w_up[0])
        gx, gg, dwg, dwd, dwu = pl.pallas_call(
            write_kernel,
            out_shape=results,
            in_specs=[vmem] * 5,
            out_specs=[hbm] * 5,
            scratch_shapes=[dma((5,))],
            compiler_params=pltpu.CompilerParams(vmem_limit_bytes=8 * 1024 * 1024),
            name='write',
        )(*outs)
        return gx, gg.T, dwg[None], dwd[None], dwu[None]

    return jax.shard_map(local_backward, mesh=mesh, in_specs=(tok_spec, tok_spec, tok_spec, tok_spec, row_spec, row_spec, row_spec, row_spec, row_spec, row_spec, row_spec), out_specs=(tok_spec, tok_spec, row_spec, row_spec, row_spec), check_vma=False)
```

```python
import functools

import jax
import jax.numpy as jnp
from jax import lax
from jax.experimental import pallas as pl
from jax.experimental.pallas import tpu as pltpu
from jax.sharding import PartitionSpec as P

MESH = pl.DeviceIdType.MESH
F32 = jnp.float32
BF16 = jnp.bfloat16
PLANES = 4
PLANE_ORDER = (1, 3, 2, 0)
NT = (((1,), (1,)), ((), ()))
TN = (((0,), (0,)), ((), ()))


def layer_kernel(cfg, go_in, eidx_in, slot_in, gates_in, x_in, hg_in, hu_in, y_in, wg_in, wd_in, wu_in,
                 gx, gg, og, od, ou,
                 go, eidx, slot, gates, send, recv, gsend, grecv, dxs, dxr, vs, vr,
                 xv, yv, hgv, huv, wgu, wd, onehot, gv, av, dhv,
                 pg, pd, pu, rg, rd, ru,
                 load_sem, wsend_sem, wrecv_sem, fsend_sem, frecv_sem, gsend_sem, grecv_sem,
                 bsend_sem, brecv_sem, vsend_sem, vrecv_sem, psend_sem, precv_sem):
    ep_n, top, tok_n, width, hidden, cap, ysz, xsz = cfg
    plane = ep_n // PLANES
    lanes = plane * cap
    rows_chunk = plane * cap
    half_d, half_f = width // 2, hidden // 2
    q = lax.axis_index('fsdp')
    me = lax.axis_index('ep')
    other = 1 - q
    my_plane = me // plane
    my_in = lax.rem(me, plane)

    def peer_in(o):
        half, i = o // (plane // 2), lax.rem(o, plane // 2)
        oy = i // (xsz // 2)
        ox = 2 * lax.rem(i, xsz // 2) + lax.rem(oy + half, 2)
        return lax.rem(my_in // xsz + oy, ysz) * xsz + lax.rem(my_in + ox, xsz)

    barrier = pltpu.get_barrier_semaphore()

    def announce(o, c):
        pl.semaphore_signal(barrier, inc=1, device_id=(q, lax.rem(me + o, ep_n)), device_id_type=MESH)
        return c

    lax.fori_loop(1, ep_n, announce, 0)
    pl.semaphore_signal(barrier, inc=1, device_id=(other, me), device_id_type=MESH)

    small = [
        pltpu.make_async_copy(src, dst, load_sem.at[7 + i])
        for i, (src, dst) in enumerate(((eidx_in, eidx), (slot_in, slot), (gates_in, gates), (go_in, go)))
    ]
    for cp in small:
        cp.start()
    loads = [
        pltpu.make_async_copy(wd_in, wd.at[pl.ds(q * half_f, half_f)], load_sem.at[0]),
        pltpu.make_async_copy(wg_in, wgu.at[pl.ds(q * half_d, half_d), pl.ds(0, hidden)], load_sem.at[1]),
        pltpu.make_async_copy(wu_in, wgu.at[pl.ds(q * half_d, half_d), pl.ds(hidden, hidden)], load_sem.at[2]),
        pltpu.make_async_copy(hg_in, hgv, load_sem.at[3]),
        pltpu.make_async_copy(hu_in, huv, load_sem.at[4]),
        pltpu.make_async_copy(y_in, yv, load_sem.at[5]),
        pltpu.make_async_copy(x_in, xv, load_sem.at[6]),
    ]
    for cp in loads:
        cp.start()

    for cp in small:
        cp.wait()
    dest = jnp.where(slot[...] >= 0, eidx[...] * cap + slot[...], ep_n * cap)
    slot_s = lax.broadcasted_iota(jnp.int32, (lanes, tok_n), 0)
    diag = lax.broadcasted_iota(jnp.int32, (lanes, lanes), 0) == lax.broadcasted_iota(jnp.int32, (lanes, lanes), 1)
    for k in range(PLANES):
        hot = jnp.zeros((lanes, tok_n), F32)
        gate = jnp.zeros((lanes, tok_n), F32)
        for j in range(top):
            hit = slot_s == dest[j:j + 1, :] - k * lanes
            hot = jnp.where(hit, 1.0, hot)
            gate = jnp.where(hit, gates[j:j + 1, :], gate)
        hot = hot.astype(BF16)
        onehot[k] = hot
        gate_col = jnp.sum(gate, axis=1, keepdims=True)
        gsend[k] = jnp.sum(jnp.where(diag, gate_col, 0.0), axis=0, keepdims=True)
        picked = jnp.dot(hot, go[...], preferred_element_type=F32)
        send[pl.ds(k * plane, plane)] = picked.reshape(plane, cap, width).astype(BF16)

    pl.semaphore_wait(barrier, ep_n)

    def partner_copy(src, dst, i, ssem, rsem):
        return pltpu.make_async_remote_copy(src_ref=src, dst_ref=dst, send_sem=ssem.at[i], recv_sem=rsem.at[i],
                                            device_id=(other, me), device_id_type=MESH)

    wcopies = [
        partner_copy(wd_in, wd.at[pl.ds(q * half_f, half_f)], 0, wsend_sem, wrecv_sem),
        partner_copy(wg_in, wgu.at[pl.ds(q * half_d, half_d), pl.ds(0, hidden)], 1, wsend_sem, wrecv_sem),
        partner_copy(wu_in, wgu.at[pl.ds(q * half_d, half_d), pl.ds(hidden, hidden)], 2, wsend_sem, wrecv_sem),
    ]
    for cp in wcopies:
        cp.start()

    def row_copy(src, dst, idx, ssem, rsem):
        return pltpu.make_async_remote_copy(src_ref=src.at[idx], dst_ref=dst.at[me], send_sem=ssem,
                                            recv_sem=rsem.at[my_plane], device_id=(q, idx), device_id_type=MESH)

    def gate_copy(idx):
        return pltpu.make_async_remote_copy(src_ref=gsend.at[idx // plane], dst_ref=grecv.at[me], send_sem=gsend_sem,
                                            recv_sem=grecv_sem.at[my_plane], device_id=(q, idx), device_id_type=MESH)

    def wait_bytes(buf, n, sem):
        part = buf.at[pl.ds(0, n)]
        pltpu.make_async_copy(part, part, sem).wait()

    def send_part(part, lo, hi, skip_own):
        first, second = PLANE_ORDER[2 * (part // 2)], PLANE_ORDER[2 * (part // 2) + 1]

        def send_one(o, c):
            for dz in (first, second):
                idx = lax.rem(my_plane + PLANES - dz, PLANES) * plane + peer_in(o)

                def go_now():
                    gate_copy(idx).start()
                    row_copy(send, recv, idx, fsend_sem.at[part], frecv_sem).start()

                if dz == 0 and skip_own:
                    pl.when(o > 0)(go_now)
                else:
                    go_now()
            return c

        lax.fori_loop(lo, hi, send_one, 0)

    half_n = plane // 2
    send_part(0, 0, half_n, False)
    send_part(1, half_n, plane, False)
    recv[me] = send[me]
    grecv[me] = gsend[my_plane]
    wait_bytes(send, plane, fsend_sem.at[0])
    send_part(2, 0, half_n, True)
    wait_bytes(send, plane, fsend_sem.at[1])
    send_part(3, half_n, plane, False)

    def wait_chunk(ci, buf, sem):
        @pl.when(ci < PLANES - 1)
        def _():
            wait_bytes(buf, plane, sem)

        @pl.when(ci == PLANES - 1)
        def _():
            wait_bytes(buf, plane - 1, sem)

    for i in (0, 1, 2):
        loads[i].wait()
        wcopies[i].wait()
    for i in (3, 4, 5):
        loads[i].wait()

    lane_c = lax.broadcasted_iota(jnp.int32, (plane, cap, lanes), 2)
    sub_c = lax.broadcasted_iota(jnp.int32, (plane, cap, lanes), 1)
    mine = lane_c == my_in * cap + sub_c

    def plane_at(ci):
        n = lax.rem(ci + 1, PLANES)
        dz = n + (n // 2) * (5 - 2 * n)
        return lax.rem(my_plane + dz, PLANES)

    def chunk(ci, c):
        zp = plane_at(ci)
        wait_chunk(ci, recv, frecv_sem.at[zp])
        wait_chunk(ci, grecv, grecv_sem.at[zp])
        rows = pl.ds(zp * rows_chunk, rows_chunk)
        blocks = pl.ds(zp * plane, plane)
        dy = recv[blocks].astype(F32).reshape(rows_chunk, width)
        gate3 = jnp.where(mine, jnp.broadcast_to(grecv[blocks], (plane, cap, lanes)), 0.0)
        gate = jnp.sum(gate3, axis=2, keepdims=True).reshape(rows_chunk, 1)
        g = (dy * gate).astype(BF16)
        gv[rows] = g
        val = jnp.sum(dy * yv[rows].astype(F32), axis=1, keepdims=True).reshape(plane, cap, 1)
        vs[blocks] = jnp.sum(jnp.where(mine, val, 0.0), axis=1, keepdims=True)
        da = lax.dot_general(g, wd[...], NT, preferred_element_type=F32)
        h1 = hgv[rows].astype(F32)
        h3 = huv[rows].astype(F32)
        sg = jax.nn.sigmoid(h1)
        silu = h1 * sg
        av[rows] = jnp.where(gate > 0.0, silu * h3, 0.0).astype(BF16)
        dhv[rows, pl.ds(0, hidden)] = (da * h3 * sg * (1.0 + h1 * (1.0 - sg))).astype(BF16)
        dhv[rows, pl.ds(hidden, hidden)] = (da * silu).astype(BF16)
        dx = lax.dot_general(dhv[rows], wgu[...], NT, preferred_element_type=F32)
        dxs[blocks] = dx.reshape(plane, cap, width).astype(BF16)

        def back_one(o, cc):
            idx = zp * plane + peer_in(o)

            @pl.when(jnp.logical_or(ci < PLANES - 1, o > 0))
            def _():
                row_copy(dxs, dxr, idx, bsend_sem, brecv_sem).start()
                row_copy(vs, vr, idx, vsend_sem, vrecv_sem).start()

            return cc

        lax.fori_loop(0, plane, back_one, 0)
        return c

    lax.fori_loop(0, PLANES, chunk, 0)
    dxr[me] = dxs[me]
    vr[me] = vs[me]

    loads[6].wait()

    def in_grads(base, to_g, to_u):
        tile = 256 if half_d % 256 == 0 else half_d

        def step(i, c):
            cols = pl.ds(pl.multiple_of(base + i * tile, tile), tile)
            r = lax.dot_general(xv[:, cols], dhv[...], TN, preferred_element_type=F32)
            to_g[pl.ds(i * tile, tile)] = r[:, :hidden]
            to_u[pl.ds(i * tile, tile)] = r[:, hidden:]
            return c

        lax.fori_loop(0, half_d // tile, step, 0)

    def out_grads(base, to_d):
        cols = pl.ds(pl.multiple_of(base, half_f), half_f)
        to_d[...] = lax.dot_general(av[:, cols], gv[...], TN, preferred_element_type=F32)

    in_grads(other * half_d, pg, pu)
    pcopies = [partner_copy(pg, rg, 0, psend_sem, precv_sem), partner_copy(pu, ru, 1, psend_sem, precv_sem)]
    pcopies[0].start()
    pcopies[1].start()
    out_grads(other * half_f, pd)
    pcopies.append(partner_copy(pd, rd, 2, psend_sem, precv_sem))
    pcopies[2].start()
    in_grads(q * half_d, og, ou)
    out_grads(q * half_f, od)
    for i, (mine_ref, got) in enumerate(((og, rg), (ou, ru), (od, rd))):
        pcopies[i].wait()
        mine_ref[...] += got[...]

    acc = jnp.zeros((tok_n, width), F32)
    vals = [jnp.zeros((lanes, tok_n), F32) for _ in range(top)]
    for ci, dz in enumerate(PLANE_ORDER):
        zp = lax.rem(my_plane + PLANES - dz, PLANES)
        n = plane - 1 if dz == 0 else plane
        wait_bytes(dxr, n, brecv_sem.at[zp])
        wait_bytes(vr, n, vrecv_sem.at[zp])
        blocks = pl.ds(zp * plane, plane)
        part = dxr[blocks].astype(F32).reshape(rows_chunk, width).astype(BF16)
        acc = acc + lax.dot_general(onehot[zp], part, TN, preferred_element_type=F32)
        back = jnp.sum(jnp.where(diag, jnp.sum(vr[blocks], axis=0), 0.0), axis=1, keepdims=True)
        for j in range(top):
            hit = slot_s == dest[j:j + 1, :] - zp * lanes
            vals[j] = jnp.where(hit, back, vals[j])
    gx[...] = acc.astype(BF16)
    for j in range(top):
        gg[j:j + 1, :] = jnp.sum(vals[j], axis=0, keepdims=True)

    wait_bytes(send, plane - 1, fsend_sem.at[2])
    wait_bytes(send, plane, fsend_sem.at[3])
    wait_bytes(grecv, ep_n - 1, gsend_sem)
    wait_bytes(dxs, ep_n - 1, bsend_sem)
    wait_bytes(vs, ep_n - 1, vsend_sem)


def write_kernel(*refs):
    n = len(refs) // 2
    sem = refs[-1]
    copies = [pltpu.make_async_copy(refs[i], refs[n + i], sem.at[i]) for i in range(n)]
    for cp in copies:
        cp.start()
    for cp in copies:
        cp.wait()


def solution(mesh):
    ep_n = mesh.shape['ep']
    tok_spec = P(('fsdp', 'ep'), None)
    row_spec = P('ep', 'fsdp', None)

    def local_backward(grad_out, expert_idx, slot_pos, gates, x_disp, h_gate, h_up, y_disp, w_gate, w_down, w_up):
        tok_n, top = expert_idx.shape
        _, rows, width = x_disp.shape
        hidden = h_gate.shape[2]
        cap = rows // ep_n
        plane = ep_n // PLANES
        ysz = 4 if plane == 16 else 2
        xsz = plane // ysz
        lanes = plane * cap
        half_d, half_f = width // 2, hidden // 2
        cfg = (ep_n, top, tok_n, width, hidden, cap, ysz, xsz)
        vmem = pl.BlockSpec(memory_space=pltpu.VMEM)
        hbm = pl.BlockSpec(memory_space=pltpu.HBM)
        dma = pltpu.SemaphoreType.DMA
        rows_buf = pltpu.VMEM((ep_n, cap, width), BF16)
        gate_buf = pltpu.VMEM((ep_n, 1, lanes), F32)
        in_part = pltpu.VMEM((half_d, hidden), F32)
        out_part = pltpu.VMEM((half_f, width), F32)
        results = [
            jax.ShapeDtypeStruct((tok_n, width), BF16),
            jax.ShapeDtypeStruct((top, tok_n), F32),
            jax.ShapeDtypeStruct((half_d, hidden), F32),
            jax.ShapeDtypeStruct((half_f, width), F32),
            jax.ShapeDtypeStruct((half_d, hidden), F32),
        ]
        outs = pl.pallas_call(
            functools.partial(layer_kernel, cfg),
            out_shape=results,
            in_specs=[hbm] * 11,
            out_specs=[vmem] * 5,
            scratch_shapes=[
                pltpu.VMEM((tok_n, width), BF16), pltpu.VMEM((top, tok_n), jnp.int32), pltpu.VMEM((top, tok_n), jnp.int32),
                pltpu.VMEM((top, tok_n), F32), rows_buf, rows_buf, pltpu.VMEM((PLANES, 1, lanes), F32), gate_buf, rows_buf, rows_buf, gate_buf, gate_buf,
                pltpu.VMEM((rows, width), BF16), pltpu.VMEM((rows, width), BF16),
                pltpu.VMEM((rows, hidden), BF16), pltpu.VMEM((rows, hidden), BF16),
                pltpu.VMEM((width, 2 * hidden), BF16), pltpu.VMEM((hidden, width), BF16),
                pltpu.VMEM((PLANES, lanes, tok_n), BF16),
                pltpu.VMEM((rows, width), BF16), pltpu.VMEM((rows, hidden), BF16), pltpu.VMEM((rows, 2 * hidden), BF16),
                in_part, out_part, in_part, in_part, out_part, in_part,
                dma((11,)), dma((3,)), dma((3,)), dma((4,)), dma((PLANES,)), dma, dma((PLANES,)),
                dma, dma((PLANES,)), dma, dma((PLANES,)), dma((3,)), dma((3,)),
            ],
            compiler_params=pltpu.CompilerParams(collective_id=0, has_side_effects=True, vmem_limit_bytes=44 * 1024 * 1024),
            name='layer',
        )(grad_out, expert_idx.T, slot_pos.T, gates.T, x_disp[0], h_gate[0], h_up[0], y_disp[0], w_gate[0], w_down[0], w_up[0])
        gx, gg, dwg, dwd, dwu = pl.pallas_call(
            write_kernel,
            out_shape=results,
            in_specs=[vmem] * 5,
            out_specs=[hbm] * 5,
            scratch_shapes=[dma((5,))],
            compiler_params=pltpu.CompilerParams(vmem_limit_bytes=8 * 1024 * 1024),
            name='write',
        )(*outs)
        return gx, gg.T, dwg[None], dwd[None], dwu[None]

    return jax.shard_map(local_backward, mesh=mesh, in_specs=(tok_spec, tok_spec, tok_spec, tok_spec, row_spec, row_spec, row_spec, row_spec, row_spec, row_spec, row_spec), out_specs=(tok_spec, tok_spec, row_spec, row_spec, row_spec), check_vma=False)
```

```python
import functools

import jax
import jax.numpy as jnp
from jax import lax
from jax.experimental import pallas as pl
from jax.experimental.pallas import tpu as pltpu
from jax.sharding import PartitionSpec as P

MESH = pl.DeviceIdType.MESH
F32 = jnp.float32
BF16 = jnp.bfloat16
PLANES = 4
PLANE_ORDER = (1, 3, 2, 0)
NT = (((1,), (1,)), ((), ()))
TN = (((0,), (0,)), ((), ()))


def layer_kernel(cfg, go_in, eidx_in, slot_in, gates_in, x_in, hg_in, hu_in, y_in, wg_in, wd_in, wu_in,
                 gx, gg, og, od, ou,
                 go, eidx, slot, gates, send, recv, gsend, grecv, dxs, dxr, vs, vr,
                 xv, yv, hgv, huv, wgu, wd, onehot, gv, av, dhv,
                 pg, pd, pu, rg, rd, ru,
                 load_sem, wsend_sem, wrecv_sem, fsend_sem, frecv_sem, gsend_sem, grecv_sem,
                 bsend_sem, brecv_sem, vsend_sem, vrecv_sem, psend_sem, precv_sem):
    ep_n, top, tok_n, width, hidden, cap, ysz, xsz = cfg
    plane = ep_n // PLANES
    lanes = plane * cap
    rows_chunk = plane * cap
    half_d, half_f = width // 2, hidden // 2
    q = lax.axis_index('fsdp')
    me = lax.axis_index('ep')
    other = 1 - q
    my_plane = me // plane
    my_in = lax.rem(me, plane)

    def peer_in(o):
        half, i = o // (plane // 2), lax.rem(o, plane // 2)
        oy = i // (xsz // 2)
        ox = 2 * lax.rem(i, xsz // 2) + lax.rem(oy + half, 2)
        return lax.rem(my_in // xsz + oy, ysz) * xsz + lax.rem(my_in + ox, xsz)

    barrier = pltpu.get_barrier_semaphore()

    def announce(o, c):
        pl.semaphore_signal(barrier, inc=1, device_id=(q, lax.rem(me + o, ep_n)), device_id_type=MESH)
        return c

    lax.fori_loop(1, ep_n, announce, 0)
    pl.semaphore_signal(barrier, inc=1, device_id=(other, me), device_id_type=MESH)

    small = [
        pltpu.make_async_copy(src, dst, load_sem.at[7 + i])
        for i, (src, dst) in enumerate(((eidx_in, eidx), (slot_in, slot), (gates_in, gates), (go_in, go)))
    ]
    for cp in small:
        cp.start()
    loads = [
        pltpu.make_async_copy(wd_in, wd.at[pl.ds(q * half_f, half_f)], load_sem.at[0]),
        pltpu.make_async_copy(wg_in, wgu.at[pl.ds(q * half_d, half_d), pl.ds(0, hidden)], load_sem.at[1]),
        pltpu.make_async_copy(wu_in, wgu.at[pl.ds(q * half_d, half_d), pl.ds(hidden, hidden)], load_sem.at[2]),
        pltpu.make_async_copy(hg_in, hgv, load_sem.at[3]),
        pltpu.make_async_copy(hu_in, huv, load_sem.at[4]),
        pltpu.make_async_copy(y_in, yv, load_sem.at[5]),
        pltpu.make_async_copy(x_in, xv, load_sem.at[6]),
    ]
    for cp in loads:
        cp.start()

    for cp in small:
        cp.wait()
    dest = jnp.where(slot[...] >= 0, eidx[...] * cap + slot[...], ep_n * cap)
    slot_s = lax.broadcasted_iota(jnp.int32, (lanes, tok_n), 0)
    diag = lax.broadcasted_iota(jnp.int32, (lanes, lanes), 0) == lax.broadcasted_iota(jnp.int32, (lanes, lanes), 1)
    for k in range(PLANES):
        hot = jnp.zeros((lanes, tok_n), F32)
        gate = jnp.zeros((lanes, tok_n), F32)
        for j in range(top):
            hit = slot_s == dest[j:j + 1, :] - k * lanes
            hot = jnp.where(hit, 1.0, hot)
            gate = jnp.where(hit, gates[j:j + 1, :], gate)
        hot = hot.astype(BF16)
        onehot[k] = hot
        gate_col = jnp.sum(gate, axis=1, keepdims=True)
        gsend[k] = jnp.sum(jnp.where(diag, gate_col, 0.0), axis=0, keepdims=True)
        picked = jnp.dot(hot, go[...], preferred_element_type=F32)
        send[pl.ds(k * plane, plane)] = picked.reshape(plane, cap, width).astype(BF16)

    pl.semaphore_wait(barrier, ep_n)

    def partner_copy(src, dst, i, ssem, rsem):
        return pltpu.make_async_remote_copy(src_ref=src, dst_ref=dst, send_sem=ssem.at[i], recv_sem=rsem.at[i],
                                            device_id=(other, me), device_id_type=MESH)

    wcopies = [
        partner_copy(wd_in, wd.at[pl.ds(q * half_f, half_f)], 0, wsend_sem, wrecv_sem),
        partner_copy(wg_in, wgu.at[pl.ds(q * half_d, half_d), pl.ds(0, hidden)], 1, wsend_sem, wrecv_sem),
        partner_copy(wu_in, wgu.at[pl.ds(q * half_d, half_d), pl.ds(hidden, hidden)], 2, wsend_sem, wrecv_sem),
    ]
    for cp in wcopies:
        cp.start()

    def row_copy(src, dst, idx, ssem, rsem):
        return pltpu.make_async_remote_copy(src_ref=src.at[idx], dst_ref=dst.at[me], send_sem=ssem,
                                            recv_sem=rsem.at[my_plane], device_id=(q, idx), device_id_type=MESH)

    def gate_copy(idx):
        return pltpu.make_async_remote_copy(src_ref=gsend.at[idx // plane], dst_ref=grecv.at[me], send_sem=gsend_sem,
                                            recv_sem=grecv_sem.at[my_plane], device_id=(q, idx), device_id_type=MESH)

    def wait_bytes(buf, n, sem):
        part = buf.at[pl.ds(0, n)]
        pltpu.make_async_copy(part, part, sem).wait()

    def send_part(part, lo, hi, skip_own):
        first, second = PLANE_ORDER[2 * (part // 2)], PLANE_ORDER[2 * (part // 2) + 1]

        def send_one(o, c):
            for dz in (first, second):
                idx = lax.rem(my_plane + PLANES - dz, PLANES) * plane + peer_in(o)

                def go_now():
                    gate_copy(idx).start()
                    row_copy(send, recv, idx, fsend_sem.at[part], frecv_sem).start()

                if dz == 0 and skip_own:
                    pl.when(o > 0)(go_now)
                else:
                    go_now()
            return c

        lax.fori_loop(lo, hi, send_one, 0)

    half_n = plane // 2
    send_part(0, 0, half_n, False)
    send_part(1, half_n, plane, False)
    recv[me] = send[me]
    grecv[me] = gsend[my_plane]
    wait_bytes(send, plane, fsend_sem.at[0])
    send_part(2, 0, half_n, True)
    wait_bytes(send, plane, fsend_sem.at[1])
    send_part(3, half_n, plane, False)

    def wait_chunk(ci, buf, sem):
        @pl.when(ci < PLANES - 1)
        def _():
            wait_bytes(buf, plane, sem)

        @pl.when(ci == PLANES - 1)
        def _():
            wait_bytes(buf, plane - 1, sem)

    for i in (0, 1, 2):
        loads[i].wait()
        wcopies[i].wait()
    for i in (3, 4, 5):
        loads[i].wait()

    lane_c = lax.broadcasted_iota(jnp.int32, (plane, cap, lanes), 2)
    sub_c = lax.broadcasted_iota(jnp.int32, (plane, cap, lanes), 1)
    mine = lane_c == my_in * cap + sub_c

    def plane_at(ci):
        n = lax.rem(ci + 1, PLANES)
        dz = n + (n // 2) * (5 - 2 * n)
        return lax.rem(my_plane + dz, PLANES)

    def chunk(ci, c):
        zp = plane_at(ci)
        wait_chunk(ci, recv, frecv_sem.at[zp])
        wait_chunk(ci, grecv, grecv_sem.at[zp])
        rows = pl.ds(zp * rows_chunk, rows_chunk)
        blocks = pl.ds(zp * plane, plane)
        dy = recv[blocks].astype(F32).reshape(rows_chunk, width)
        gate3 = jnp.where(mine, jnp.broadcast_to(grecv[blocks], (plane, cap, lanes)), 0.0)
        gate = jnp.sum(gate3, axis=2, keepdims=True).reshape(rows_chunk, 1)
        g = (dy * gate).astype(BF16)
        gv[rows] = g
        val = jnp.sum(dy * yv[rows].astype(F32), axis=1, keepdims=True).reshape(plane, cap, 1)
        vs[blocks] = jnp.sum(jnp.where(mine, val, 0.0), axis=1, keepdims=True)
        da = lax.dot_general(g, wd[...], NT, preferred_element_type=F32)
        h1 = hgv[rows].astype(F32)
        h3 = huv[rows].astype(F32)
        sg = jax.nn.sigmoid(h1)
        silu = h1 * sg
        av[rows] = jnp.where(gate > 0.0, silu * h3, 0.0).astype(BF16)
        dhv[rows, pl.ds(0, hidden)] = (da * h3 * sg * (1.0 + h1 * (1.0 - sg))).astype(BF16)
        dhv[rows, pl.ds(hidden, hidden)] = (da * silu).astype(BF16)
        dx = lax.dot_general(dhv[rows], wgu[...], NT, preferred_element_type=F32)
        dxs[blocks] = dx.reshape(plane, cap, width).astype(BF16)

        def back_one(o, cc):
            idx = zp * plane + peer_in(o)

            @pl.when(jnp.logical_or(ci < PLANES - 1, o > 0))
            def _():
                row_copy(dxs, dxr, idx, bsend_sem, brecv_sem).start()
                row_copy(vs, vr, idx, vsend_sem, vrecv_sem).start()

            return cc

        lax.fori_loop(0, plane, back_one, 0)
        return c

    lax.fori_loop(0, PLANES, chunk, 0)
    dxr[me] = dxs[me]
    vr[me] = vs[me]

    loads[6].wait()

    def in_grads(base, to_g, to_u):
        tile = 256 if half_d % 256 == 0 else half_d

        def step(i, c):
            cols = pl.ds(pl.multiple_of(base + i * tile, tile), tile)
            r = lax.dot_general(xv[:, cols], dhv[...], TN, preferred_element_type=F32)
            to_g[pl.ds(i * tile, tile)] = r[:, :hidden]
            to_u[pl.ds(i * tile, tile)] = r[:, hidden:]
            return c

        lax.fori_loop(0, half_d // tile, step, 0)

    def out_grads(base, to_d):
        cols = pl.ds(pl.multiple_of(base, half_f), half_f)
        to_d[...] = lax.dot_general(av[:, cols], gv[...], TN, preferred_element_type=F32)

    in_grads(other * half_d, pg, pu)
    pcopies = [partner_copy(pg, rg, 0, psend_sem, precv_sem), partner_copy(pu, ru, 1, psend_sem, precv_sem)]
    pcopies[0].start()
    pcopies[1].start()
    out_grads(other * half_f, pd)
    pcopies.append(partner_copy(pd, rd, 2, psend_sem, precv_sem))
    pcopies[2].start()
    in_grads(q * half_d, og, ou)
    out_grads(q * half_f, od)
    for i, (mine_ref, got) in enumerate(((og, rg), (ou, ru), (od, rd))):
        pcopies[i].wait()
        mine_ref[...] += got[...]

    acc = jnp.zeros((tok_n, width), F32)
    vals = [jnp.zeros((lanes, tok_n), F32) for _ in range(top)]
    for ci, dz in enumerate(PLANE_ORDER):
        zp = lax.rem(my_plane + PLANES - dz, PLANES)
        n = plane - 1 if dz == 0 else plane
        wait_bytes(dxr, n, brecv_sem.at[zp])
        wait_bytes(vr, n, vrecv_sem.at[zp])
        blocks = pl.ds(zp * plane, plane)
        part = dxr[blocks].astype(F32).reshape(rows_chunk, width).astype(BF16)
        acc = acc + lax.dot_general(onehot[zp], part, TN, preferred_element_type=F32)
        back = jnp.sum(jnp.where(diag, jnp.sum(vr[blocks], axis=0), 0.0), axis=1, keepdims=True)
        for j in range(top):
            hit = slot_s == dest[j:j + 1, :] - zp * lanes
            vals[j] = jnp.where(hit, back, vals[j])
    gx[...] = acc.astype(BF16)
    for j in range(top):
        gg[j:j + 1, :] = jnp.sum(vals[j], axis=0, keepdims=True)

    wait_bytes(send, plane - 1, fsend_sem.at[2])
    wait_bytes(send, plane, fsend_sem.at[3])
    wait_bytes(grecv, ep_n - 1, gsend_sem)
    wait_bytes(dxs, ep_n - 1, bsend_sem)
    wait_bytes(vs, ep_n - 1, vsend_sem)


def write_kernel(*refs):
    n = len(refs) // 2
    sem = refs[-1]
    copies = [pltpu.make_async_copy(refs[i], refs[n + i], sem.at[i]) for i in range(n)]
    for cp in copies:
        cp.start()
    for cp in copies:
        cp.wait()


def solution(mesh):
    ep_n = mesh.shape['ep']
    tok_spec = P(('fsdp', 'ep'), None)
    row_spec = P('ep', 'fsdp', None)

    def local_backward(grad_out, expert_idx, slot_pos, gates, x_disp, h_gate, h_up, y_disp, w_gate, w_down, w_up):
        tok_n, top = expert_idx.shape
        _, rows, width = x_disp.shape
        hidden = h_gate.shape[2]
        cap = rows // ep_n
        plane = ep_n // PLANES
        ysz = 4 if plane == 16 else 2
        xsz = plane // ysz
        lanes = plane * cap
        half_d, half_f = width // 2, hidden // 2
        cfg = (ep_n, top, tok_n, width, hidden, cap, ysz, xsz)
        vmem = pl.BlockSpec(memory_space=pltpu.VMEM)
        hbm = pl.BlockSpec(memory_space=pltpu.HBM)
        dma = pltpu.SemaphoreType.DMA
        rows_buf = pltpu.VMEM((ep_n, cap, width), BF16)
        gate_buf = pltpu.VMEM((ep_n, 1, lanes), F32)
        in_part = pltpu.VMEM((half_d, hidden), F32)
        out_part = pltpu.VMEM((half_f, width), F32)
        results = [
            jax.ShapeDtypeStruct((tok_n, width), BF16),
            jax.ShapeDtypeStruct((top, tok_n), F32),
            jax.ShapeDtypeStruct((half_d, hidden), F32),
            jax.ShapeDtypeStruct((half_f, width), F32),
            jax.ShapeDtypeStruct((half_d, hidden), F32),
        ]
        outs = pl.pallas_call(
            functools.partial(layer_kernel, cfg),
            out_shape=results,
            in_specs=[hbm] * 11,
            out_specs=[vmem] * 5,
            scratch_shapes=[
                pltpu.VMEM((tok_n, width), BF16), pltpu.VMEM((top, tok_n), jnp.int32), pltpu.VMEM((top, tok_n), jnp.int32),
                pltpu.VMEM((top, tok_n), F32), rows_buf, rows_buf, pltpu.VMEM((PLANES, 1, lanes), F32), gate_buf, rows_buf, rows_buf, gate_buf, gate_buf,
                pltpu.VMEM((rows, width), BF16), pltpu.VMEM((rows, width), BF16),
                pltpu.VMEM((rows, hidden), BF16), pltpu.VMEM((rows, hidden), BF16),
                pltpu.VMEM((width, 2 * hidden), BF16), pltpu.VMEM((hidden, width), BF16),
                pltpu.VMEM((PLANES, lanes, tok_n), BF16),
                pltpu.VMEM((rows, width), BF16), pltpu.VMEM((rows, hidden), BF16), pltpu.VMEM((rows, 2 * hidden), BF16),
                in_part, out_part, in_part, in_part, out_part, in_part,
                dma((11,)), dma((3,)), dma((3,)), dma((4,)), dma((PLANES,)), dma, dma((PLANES,)),
                dma, dma((PLANES,)), dma, dma((PLANES,)), dma((3,)), dma((3,)),
            ],
            compiler_params=pltpu.CompilerParams(collective_id=0, has_side_effects=True, vmem_limit_bytes=44 * 1024 * 1024),
            name='layer',
        )(*[pltpu.with_memory_space_constraint(v, pltpu.HBM) for v in (grad_out, expert_idx.T, slot_pos.T, gates.T, x_disp[0], h_gate[0], h_up[0], y_disp[0], w_gate[0], w_down[0], w_up[0])])
        gx, gg, dwg, dwd, dwu = pl.pallas_call(
            write_kernel,
            out_shape=results,
            in_specs=[vmem] * 5,
            out_specs=[hbm] * 5,
            scratch_shapes=[dma((5,))],
            compiler_params=pltpu.CompilerParams(vmem_limit_bytes=8 * 1024 * 1024),
            name='write',
        )(*outs)
        return gx, gg.T, dwg[None], dwd[None], dwu[None]

    return jax.shard_map(local_backward, mesh=mesh, in_specs=(tok_spec, tok_spec, tok_spec, tok_spec, row_spec, row_spec, row_spec, row_spec, row_spec, row_spec, row_spec), out_specs=(tok_spec, tok_spec, row_spec, row_spec, row_spec), check_vma=False)
```

```python
import functools

import jax
import jax.numpy as jnp
from jax import lax
from jax.experimental import pallas as pl
from jax.experimental.pallas import tpu as pltpu
from jax.sharding import PartitionSpec as P

MESH = pl.DeviceIdType.MESH
F32 = jnp.float32
BF16 = jnp.bfloat16
PLANES = 4
ORDERS = {'near': (1, 3, 2, 0), 'far': (2, 3, 1, 0)}
NT = (((1,), (1,)), ((), ()))
TN = (((0,), (0,)), ((), ()))


OPT = dict(order='near', mirror=False)


def layer_kernel(cfg, opt, go_in, eidx_in, slot_in, gates_in, x_in, hg_in, hu_in, y_in, wg_in, wd_in, wu_in,
                 gx, gg, og, od, ou,
                 go, eidx, slot, gates, send, recv, gsend, gz, grecv, dxs, dxr, vs, vr, vsum, back4,
                 xv, yv, hgv, huv, wgu, wd, onehot, gv, av, dhv,
                 pg, pd, pu, rg, rd, ru,
                 load_sem, wsend_sem, wrecv_sem, fsend_sem, frecv_sem, gsend_sem, grecv_sem,
                 bsend_sem, brecv_sem, vsend_sem, vrecv_sem, psend_sem, precv_sem):
    ep_n, top, tok_n, width, hidden, cap, ysz, xsz = cfg
    PLANE_ORDER = ORDERS[opt['order']]
    plane = ep_n // PLANES
    lanes = plane * cap
    rows_chunk = plane * cap
    half_d, half_f = width // 2, hidden // 2
    q = lax.axis_index('fsdp')
    me = lax.axis_index('ep')
    other = 1 - q
    my_plane = me // plane
    my_in = lax.rem(me, plane)

    def peer_in(o):
        half, i = o // (plane // 2), lax.rem(o, plane // 2)
        oy = i // (xsz // 2)
        ox = 2 * lax.rem(i, xsz // 2) + lax.rem(oy + half, 2)
        my_y, my_x = my_in // xsz, lax.rem(my_in, xsz)
        if opt['mirror']:
            oy = oy + lax.rem(my_y, 2) * (ysz - 2 * oy)
            ox = ox + lax.rem(my_x, 2) * (xsz - 2 * ox)
        return lax.rem(my_y + oy, ysz) * xsz + lax.rem(my_x + ox, xsz)

    barrier = pltpu.get_barrier_semaphore()

    def announce(o, c):
        pl.semaphore_signal(barrier, inc=1, device_id=(q, lax.rem(me + o, ep_n)), device_id_type=MESH)
        return c

    lax.fori_loop(1, ep_n, announce, 0)
    pl.semaphore_signal(barrier, inc=1, device_id=(other, me), device_id_type=MESH)

    small = [
        pltpu.make_async_copy(src, dst, load_sem.at[7 + i])
        for i, (src, dst) in enumerate(((eidx_in, eidx), (slot_in, slot), (gates_in, gates), (go_in, go)))
    ]
    for cp in small:
        cp.start()
    loads = [
        pltpu.make_async_copy(wd_in, wd.at[pl.ds(q * half_f, half_f)], load_sem.at[0]),
        pltpu.make_async_copy(wg_in, wgu.at[pl.ds(q * half_d, half_d), pl.ds(0, hidden)], load_sem.at[1]),
        pltpu.make_async_copy(wu_in, wgu.at[pl.ds(q * half_d, half_d), pl.ds(hidden, hidden)], load_sem.at[2]),
        pltpu.make_async_copy(hg_in, hgv, load_sem.at[3]),
        pltpu.make_async_copy(hu_in, huv, load_sem.at[4]),
        pltpu.make_async_copy(y_in, yv, load_sem.at[5]),
        pltpu.make_async_copy(x_in, xv, load_sem.at[6]),
    ]
    for cp in loads:
        cp.start()

    for cp in small:
        cp.wait()
    dest = jnp.where(slot[...] >= 0, eidx[...] * cap + slot[...], ep_n * cap)
    slot_s = lax.broadcasted_iota(jnp.int32, (lanes, tok_n), 0)
    diag = lax.broadcasted_iota(jnp.int32, (lanes, lanes), 0) == lax.broadcasted_iota(jnp.int32, (lanes, lanes), 1)
    for k in range(PLANES):
        hot = jnp.zeros((lanes, tok_n), F32)
        gate = jnp.zeros((lanes, tok_n), F32)
        for j in range(top):
            hit = slot_s == dest[j:j + 1, :] - k * lanes
            hot = jnp.where(hit, 1.0, hot)
            gate = jnp.where(hit, gates[j:j + 1, :], gate)
        hot = hot.astype(BF16)
        onehot[k] = hot
        gate_col = jnp.sum(gate, axis=1, keepdims=True)
        gsend[k] = jnp.sum(jnp.where(diag, gate_col, 0.0), axis=0, keepdims=True)
        picked = jnp.dot(hot, go[...], preferred_element_type=F32)
        send[pl.ds(k * plane, plane)] = picked.reshape(plane, cap, width).astype(BF16)

    pl.semaphore_wait(barrier, ep_n)

    def partner_copy(src, dst, i, ssem, rsem):
        return pltpu.make_async_remote_copy(src_ref=src, dst_ref=dst, send_sem=ssem.at[i], recv_sem=rsem.at[i],
                                            device_id=(other, me), device_id_type=MESH)

    wcopies = [
        partner_copy(wd_in, wd.at[pl.ds(q * half_f, half_f)], 0, wsend_sem, wrecv_sem),
        partner_copy(wg_in, wgu.at[pl.ds(q * half_d, half_d), pl.ds(0, hidden)], 1, wsend_sem, wrecv_sem),
        partner_copy(wu_in, wgu.at[pl.ds(q * half_d, half_d), pl.ds(hidden, hidden)], 2, wsend_sem, wrecv_sem),
    ]
    for cp in wcopies:
        cp.start()

    def row_copy(src, dst, idx, ssem, rsem):
        return pltpu.make_async_remote_copy(src_ref=src.at[idx], dst_ref=dst.at[me], send_sem=ssem,
                                            recv_sem=rsem.at[my_plane], device_id=(q, idx), device_id_type=MESH)

    def line_copy(dz, src, dst, ssem, rsem):
        zt = lax.rem(my_plane + dz, PLANES)
        return pltpu.make_async_remote_copy(src_ref=src.at[zt], dst_ref=dst.at[my_plane], send_sem=ssem, recv_sem=rsem,
                                            device_id=(q, zt * plane + my_in), device_id_type=MESH)

    def in_plane_copy(o, src, dst, ssem, rsem):
        to = peer_in(o)
        part = src if len(src.shape) == 3 else src.at[to]
        return pltpu.make_async_remote_copy(src_ref=part, dst_ref=dst.at[my_in], send_sem=ssem, recv_sem=rsem,
                                            device_id=(q, my_plane * plane + to), device_id_type=MESH)

    def wait_bytes(buf, n, sem):
        part = buf.at[pl.ds(0, n)]
        pltpu.make_async_copy(part, part, sem).wait()

    def send_part(part, lo, hi, skip_own):
        first, second = PLANE_ORDER[2 * (part // 2)], PLANE_ORDER[2 * (part // 2) + 1]

        def send_one(o, c):
            for dz in (first, second):
                idx = lax.rem(my_plane + PLANES - dz, PLANES) * plane + peer_in(o)

                def go_now():
                    row_copy(send, recv, idx, fsend_sem.at[part], frecv_sem).start()

                if dz == 0 and skip_own:
                    pl.when(o > 0)(go_now)
                else:
                    go_now()
            return c

        lax.fori_loop(lo, hi, send_one, 0)

    half_n = plane // 2
    for dz in range(1, PLANES):
        line_copy(dz, gsend, gz, gsend_sem.at[0], grecv_sem.at[0]).start()
    send_part(0, 0, half_n, False)
    recv[me] = send[me]
    gz[my_plane] = gsend[my_plane]
    wait_bytes(gz, PLANES - 1, grecv_sem.at[0])

    def spread(o, c):
        in_plane_copy(o, gz, grecv, gsend_sem.at[1], grecv_sem.at[1]).start()
        return c

    lax.fori_loop(1, plane, spread, 0)
    grecv[my_in] = gz[...]
    send_part(1, half_n, plane, False)
    send_part(2, 0, half_n, True)
    send_part(3, half_n, plane, False)

    def wait_chunk(ci, buf, sem):
        @pl.when(ci < PLANES - 1)
        def _():
            wait_bytes(buf, plane, sem)

        @pl.when(ci == PLANES - 1)
        def _():
            wait_bytes(buf, plane - 1, sem)

    for i in (0, 1, 2):
        loads[i].wait()
        wcopies[i].wait()
    for i in (3, 4, 5):
        loads[i].wait()
    wait_bytes(grecv, plane - 1, grecv_sem.at[1])

    lane_c = lax.broadcasted_iota(jnp.int32, (plane, cap, lanes), 2)
    sub_c = lax.broadcasted_iota(jnp.int32, (plane, cap, lanes), 1)
    mine = lane_c == my_in * cap + sub_c

    def plane_at(ci):
        n = lax.rem(ci + 1, PLANES) if opt['order'] == 'near' else PLANES - 1 - ci
        dz = n + (n // 2) * (5 - 2 * n)
        return lax.rem(my_plane + dz, PLANES)

    def chunk(ci, c):
        zp = plane_at(ci)
        wait_chunk(ci, recv, frecv_sem.at[zp])
        rows = pl.ds(zp * rows_chunk, rows_chunk)
        blocks = pl.ds(zp * plane, plane)
        dy = recv[blocks].astype(F32).reshape(rows_chunk, width)
        gate3 = jnp.where(mine, jnp.broadcast_to(grecv[:, zp], (plane, cap, lanes)), 0.0)
        gate = jnp.sum(gate3, axis=2, keepdims=True).reshape(rows_chunk, 1)
        g = (dy * gate).astype(BF16)
        gv[rows] = g
        val = jnp.sum(dy * yv[rows].astype(F32), axis=1, keepdims=True).reshape(plane, cap, 1)
        vs[:, zp] = jnp.sum(jnp.where(mine, val, 0.0), axis=1, keepdims=True)

        @pl.when(ci == PLANES - 1)
        def _():
            def gather_back(o, cc):
                in_plane_copy(o, vs, vr, vsend_sem.at[0], vrecv_sem.at[0]).start()
                return cc

            lax.fori_loop(1, plane, gather_back, 0)

        da = lax.dot_general(g, wd[...], NT, preferred_element_type=F32)
        h1 = hgv[rows].astype(F32)
        h3 = huv[rows].astype(F32)
        sg = jax.nn.sigmoid(h1)
        silu = h1 * sg
        av[rows] = jnp.where(gate > 0.0, silu * h3, 0.0).astype(BF16)
        dhv[rows, pl.ds(0, hidden)] = (da * h3 * sg * (1.0 + h1 * (1.0 - sg))).astype(BF16)
        dhv[rows, pl.ds(hidden, hidden)] = (da * silu).astype(BF16)
        dx = lax.dot_general(dhv[rows], wgu[...], NT, preferred_element_type=F32)
        dxs[blocks] = dx.reshape(plane, cap, width).astype(BF16)

        def back_one(o, cc):
            idx = zp * plane + peer_in(o)

            @pl.when(jnp.logical_or(ci < PLANES - 1, o > 0))
            def _():
                row_copy(dxs, dxr, idx, bsend_sem, brecv_sem).start()

            return cc

        lax.fori_loop(0, plane, back_one, 0)
        return c

    lax.fori_loop(0, PLANES, chunk, 0)
    dxr[me] = dxs[me]
    vr[my_in] = vs[my_in]

    loads[6].wait()

    def in_grads(base, to_g, to_u):
        tile = 256 if half_d % 256 == 0 else half_d

        def step(i, c):
            cols = pl.ds(pl.multiple_of(base + i * tile, tile), tile)
            r = lax.dot_general(xv[:, cols], dhv[...], TN, preferred_element_type=F32)
            to_g[pl.ds(i * tile, tile)] = r[:, :hidden]
            to_u[pl.ds(i * tile, tile)] = r[:, hidden:]
            return c

        lax.fori_loop(0, half_d // tile, step, 0)

    def out_grads(base, to_d):
        cols = pl.ds(pl.multiple_of(base, half_f), half_f)
        to_d[...] = lax.dot_general(av[:, cols], gv[...], TN, preferred_element_type=F32)

    in_grads(other * half_d, pg, pu)
    pcopies = [partner_copy(pg, rg, 0, psend_sem, precv_sem), partner_copy(pu, ru, 1, psend_sem, precv_sem)]
    pcopies[0].start()
    pcopies[1].start()
    out_grads(other * half_f, pd)
    pcopies.append(partner_copy(pd, rd, 2, psend_sem, precv_sem))
    pcopies[2].start()
    in_grads(q * half_d, og, ou)
    wait_bytes(vr, plane - 1, vrecv_sem.at[0])
    total = jnp.sum(vr[...], axis=0)
    vsum[...] = total
    back4[my_plane] = vsum[my_plane]
    out_grads(q * half_f, od)
    for dz in range(1, PLANES):
        line_copy(dz, vsum, back4, vsend_sem.at[1], vrecv_sem.at[1]).start()
    for i, (mine_ref, got) in enumerate(((og, rg), (ou, ru), (od, rd))):
        pcopies[i].wait()
        mine_ref[...] += got[...]

    wait_bytes(back4, PLANES - 1, vrecv_sem.at[1])
    acc = jnp.zeros((tok_n, width), F32)
    vals = [jnp.zeros((lanes, tok_n), F32) for _ in range(top)]
    for ci, dz in enumerate(PLANE_ORDER):
        zp = lax.rem(my_plane + PLANES - dz, PLANES)
        n = plane - 1 if dz == 0 else plane
        wait_bytes(dxr, n, brecv_sem.at[zp])
        blocks = pl.ds(zp * plane, plane)
        part = dxr[blocks].astype(F32).reshape(rows_chunk, width).astype(BF16)
        acc = acc + lax.dot_general(onehot[zp], part, TN, preferred_element_type=F32)
        back = jnp.sum(jnp.where(diag, back4[zp], 0.0), axis=1, keepdims=True)
        for j in range(top):
            hit = slot_s == dest[j:j + 1, :] - zp * lanes
            vals[j] = jnp.where(hit, back, vals[j])
    gx[...] = acc.astype(BF16)
    for j in range(top):
        gg[j:j + 1, :] = jnp.sum(vals[j], axis=0, keepdims=True)

    wait_bytes(send, plane - 1, fsend_sem.at[2])
    wait_bytes(send, plane, fsend_sem.at[3])
    wait_bytes(send, plane, fsend_sem.at[0])
    wait_bytes(send, plane, fsend_sem.at[1])
    wait_bytes(gz, PLANES - 1, gsend_sem.at[0])
    wait_bytes(grecv, plane - 1, gsend_sem.at[1])
    wait_bytes(dxs, ep_n - 1, bsend_sem)
    wait_bytes(vr, plane - 1, vsend_sem.at[0])
    wait_bytes(back4, PLANES - 1, vsend_sem.at[1])


def write_kernel(*refs):
    n = len(refs) // 2
    sem = refs[-1]
    copies = [pltpu.make_async_copy(refs[i], refs[n + i], sem.at[i]) for i in range(n)]
    for cp in copies:
        cp.start()
    for cp in copies:
        cp.wait()


def solution(mesh):
    ep_n = mesh.shape['ep']
    tok_spec = P(('fsdp', 'ep'), None)
    row_spec = P('ep', 'fsdp', None)

    def local_backward(grad_out, expert_idx, slot_pos, gates, x_disp, h_gate, h_up, y_disp, w_gate, w_down, w_up):
        tok_n, top = expert_idx.shape
        _, rows, width = x_disp.shape
        hidden = h_gate.shape[2]
        cap = rows // ep_n
        plane = ep_n // PLANES
        ysz = 4 if plane == 16 else 2
        xsz = plane // ysz
        lanes = plane * cap
        half_d, half_f = width // 2, hidden // 2
        cfg = (ep_n, top, tok_n, width, hidden, cap, ysz, xsz)
        vmem = pl.BlockSpec(memory_space=pltpu.VMEM)
        hbm = pl.BlockSpec(memory_space=pltpu.HBM)
        dma = pltpu.SemaphoreType.DMA
        rows_buf = pltpu.VMEM((ep_n, cap, width), BF16)
        line_buf = pltpu.VMEM((PLANES, 1, lanes), F32)
        gate_buf = pltpu.VMEM((plane, PLANES, 1, lanes), F32)
        in_part = pltpu.VMEM((half_d, hidden), F32)
        out_part = pltpu.VMEM((half_f, width), F32)
        results = [
            jax.ShapeDtypeStruct((tok_n, width), BF16),
            jax.ShapeDtypeStruct((top, tok_n), F32),
            jax.ShapeDtypeStruct((half_d, hidden), F32),
            jax.ShapeDtypeStruct((half_f, width), F32),
            jax.ShapeDtypeStruct((half_d, hidden), F32),
        ]
        outs = pl.pallas_call(
            functools.partial(layer_kernel, cfg, OPT),
            out_shape=results,
            in_specs=[hbm] * 11,
            out_specs=[vmem] * 5,
            scratch_shapes=[
                pltpu.VMEM((tok_n, width), BF16), pltpu.VMEM((top, tok_n), jnp.int32), pltpu.VMEM((top, tok_n), jnp.int32),
                pltpu.VMEM((top, tok_n), F32), rows_buf, rows_buf, line_buf, line_buf, gate_buf, rows_buf, rows_buf, gate_buf, gate_buf, line_buf, line_buf,
                pltpu.VMEM((rows, width), BF16), pltpu.VMEM((rows, width), BF16),
                pltpu.VMEM((rows, hidden), BF16), pltpu.VMEM((rows, hidden), BF16),
                pltpu.VMEM((width, 2 * hidden), BF16), pltpu.VMEM((hidden, width), BF16),
                pltpu.VMEM((PLANES, lanes, tok_n), BF16),
                pltpu.VMEM((rows, width), BF16), pltpu.VMEM((rows, hidden), BF16), pltpu.VMEM((rows, 2 * hidden), BF16),
                in_part, out_part, in_part, in_part, out_part, in_part,
                dma((11,)), dma((3,)), dma((3,)), dma((4,)), dma((PLANES,)), dma((2,)), dma((2,)),
                dma, dma((PLANES,)), dma((2,)), dma((2,)), dma((3,)), dma((3,)),
            ],
            compiler_params=pltpu.CompilerParams(collective_id=0, has_side_effects=True, vmem_limit_bytes=44 * 1024 * 1024),
            name='layer',
        )(*[pltpu.with_memory_space_constraint(v, pltpu.HBM) for v in (grad_out, expert_idx.T, slot_pos.T, gates.T, x_disp[0], h_gate[0], h_up[0], y_disp[0], w_gate[0], w_down[0], w_up[0])])
        gx, gg, dwg, dwd, dwu = pl.pallas_call(
            write_kernel,
            out_shape=results,
            in_specs=[vmem] * 5,
            out_specs=[hbm] * 5,
            scratch_shapes=[dma((5,))],
            compiler_params=pltpu.CompilerParams(vmem_limit_bytes=8 * 1024 * 1024),
            name='write',
        )(*outs)
        return gx, gg.T, dwg[None], dwd[None], dwu[None]

    return jax.shard_map(local_backward, mesh=mesh, in_specs=(tok_spec, tok_spec, tok_spec, tok_spec, row_spec, row_spec, row_spec, row_spec, row_spec, row_spec, row_spec), out_specs=(tok_spec, tok_spec, row_spec, row_spec, row_spec), check_vma=False)
```

```python
import functools

import jax
import jax.numpy as jnp
from jax import lax
from jax.experimental import pallas as pl
from jax.experimental.pallas import tpu as pltpu
from jax.sharding import PartitionSpec as P

MESH = pl.DeviceIdType.MESH
F32 = jnp.float32
BF16 = jnp.bfloat16
PLANES = 4
NT = (((1,), (1,)), ((), ()))
TN = (((0,), (0,)), ((), ()))


def layer_kernel(cfg, go_in, eidx_in, slot_in, gates_in, x_in, hg_in, hu_in, y_in, wg_in, wd_in, wu_in,
                 gx, gg, og, od, ou,
                 go, eidx, slot, gates, send, recv, gsend, gz, grecv, dxs, dxr, vs, vr, vsum, back4,
                 xv, yv, hgv, huv, wgu, wd, onehot, gv, av, dhv,
                 pg, pd, pu, rg, rd, ru,
                 load_sem, wsend_sem, wrecv_sem, fsend_sem, frecv_sem, gsend_sem, grecv_sem,
                 bsend_sem, brecv_sem, vsend_sem, vrecv_sem, psend_sem, precv_sem):
    ep_n, top, tok_n, width, hidden, cap, ysz, xsz = cfg
    plane = ep_n // PLANES
    lanes = plane * cap
    rows_chunk = plane * cap
    half_d, half_f = width // 2, hidden // 2
    q = lax.axis_index('fsdp')
    me = lax.axis_index('ep')
    other = 1 - q
    my_plane = me // plane
    my_in = lax.rem(me, plane)

    my_y, my_x = my_in // xsz, lax.rem(my_in, xsz)

    def walk(c, k, n):
        return lax.rem(c + (1 - 2 * lax.rem(c, 2)) * k + n, n)

    def peer_in(o):
        return walk(my_y, o // xsz, ysz) * xsz + walk(my_x, lax.rem(o, xsz), xsz)

    def peer(pos):
        o = lax.rem(pos, plane)
        dz = lax.rem(o // xsz + lax.rem(o, xsz) + pos // plane, PLANES)
        return walk(my_plane, dz, PLANES), peer_in(o)

    barrier = pltpu.get_barrier_semaphore()

    def announce(o, c):
        pl.semaphore_signal(barrier, inc=1, device_id=(q, lax.rem(me + o, ep_n)), device_id_type=MESH)
        return c

    lax.fori_loop(1, ep_n, announce, 0)
    pl.semaphore_signal(barrier, inc=1, device_id=(other, me), device_id_type=MESH)

    small = [
        pltpu.make_async_copy(src, dst, load_sem.at[7 + i])
        for i, (src, dst) in enumerate(((eidx_in, eidx), (slot_in, slot), (gates_in, gates), (go_in, go)))
    ]
    for cp in small:
        cp.start()
    loads = [
        pltpu.make_async_copy(wd_in, wd.at[pl.ds(q * half_f, half_f)], load_sem.at[0]),
        pltpu.make_async_copy(wg_in, wgu.at[pl.ds(q * half_d, half_d), pl.ds(0, hidden)], load_sem.at[1]),
        pltpu.make_async_copy(wu_in, wgu.at[pl.ds(q * half_d, half_d), pl.ds(hidden, hidden)], load_sem.at[2]),
    ]
    for cp in loads:
        cp.start()

    for cp in small:
        cp.wait()
    kept = slot[...] >= 0
    dest = jnp.where(kept, eidx[...] * cap + slot[...], ep_n * cap)

    def steps(place, c, n):
        return ((1 - 2 * lax.rem(c, 2)) * (place - c) + 2 * n) & (n - 1)

    place_in = eidx[...] & (plane - 1)
    dz = steps(eidx[...] >> (plane.bit_length() - 1), my_plane, PLANES)
    dy = steps(place_in >> (xsz.bit_length() - 1), my_y, ysz)
    dx = steps(place_in & (xsz - 1), my_x, xsz)
    pos_of = ((dz - dy - dx + 2 * PLANES) & (PLANES - 1)) * plane + dy * xsz + dx
    dest_pos = jnp.where(kept, pos_of * cap + slot[...], ep_n * cap)
    slot_s = lax.broadcasted_iota(jnp.int32, (lanes, tok_n), 0)
    diag = lax.broadcasted_iota(jnp.int32, (lanes, lanes), 0) == lax.broadcasted_iota(jnp.int32, (lanes, lanes), 1)
    for k in range(PLANES):
        hot = jnp.zeros((lanes, tok_n), F32)
        gate = jnp.zeros((lanes, tok_n), F32)
        for j in range(top):
            hot = jnp.where(slot_s == dest_pos[j:j + 1, :] - k * lanes, 1.0, hot)
            gate = jnp.where(slot_s == dest[j:j + 1, :] - k * lanes, gates[j:j + 1, :], gate)
        hot = hot.astype(BF16)
        onehot[k] = hot
        gate_col = jnp.sum(gate, axis=1, keepdims=True)
        gsend[k] = jnp.sum(jnp.where(diag, gate_col, 0.0), axis=0, keepdims=True)
        picked = jnp.dot(hot, go[...], preferred_element_type=F32)
        send[pl.ds(k * plane, plane)] = picked.reshape(plane, cap, width).astype(BF16)

    pl.semaphore_wait(barrier, ep_n)

    def partner_copy(src, dst, i, ssem, rsem):
        return pltpu.make_async_remote_copy(src_ref=src, dst_ref=dst, send_sem=ssem.at[i], recv_sem=rsem.at[i],
                                            device_id=(other, me), device_id_type=MESH)

    wcopies = [
        partner_copy(wd_in, wd.at[pl.ds(q * half_f, half_f)], 0, wsend_sem, wrecv_sem),
        partner_copy(wg_in, wgu.at[pl.ds(q * half_d, half_d), pl.ds(0, hidden)], 1, wsend_sem, wrecv_sem),
        partner_copy(wu_in, wgu.at[pl.ds(q * half_d, half_d), pl.ds(hidden, hidden)], 2, wsend_sem, wrecv_sem),
    ]
    for cp in wcopies:
        cp.start()

    def row_copy(src, dst, pos, ssem, rsem):
        zt, it = peer(pos)
        return pltpu.make_async_remote_copy(src_ref=src.at[pos], dst_ref=dst.at[pos], send_sem=ssem,
                                            recv_sem=rsem.at[pos // plane], device_id=(q, zt * plane + it), device_id_type=MESH)

    def line_copy(dz, src, dst, ssem, rsem):
        zt = lax.rem(my_plane + dz, PLANES)
        return pltpu.make_async_remote_copy(src_ref=src.at[zt], dst_ref=dst.at[my_plane], send_sem=ssem, recv_sem=rsem,
                                            device_id=(q, zt * plane + my_in), device_id_type=MESH)

    def in_plane_copy(o, src, dst, ssem, rsem):
        to = peer_in(o)
        part = src if len(src.shape) == 3 else src.at[to]
        return pltpu.make_async_remote_copy(src_ref=part, dst_ref=dst.at[my_in], send_sem=ssem, recv_sem=rsem,
                                            device_id=(q, my_plane * plane + to), device_id_type=MESH)

    def wait_bytes(buf, n, sem):
        part = buf.at[pl.ds(0, n)]
        pltpu.make_async_copy(part, part, sem).wait()

    def send_rows(lo, hi):
        def send_one(pos, c):
            row_copy(send, recv, pos, fsend_sem, frecv_sem).start()
            return c

        lax.fori_loop(lo, hi, send_one, 0)

    for dz in range(1, PLANES):
        line_copy(dz, gsend, gz, gsend_sem.at[0], grecv_sem.at[0]).start()
    send_rows(1, plane)
    recv[0] = send[0]
    gz[my_plane] = gsend[my_plane]
    wait_bytes(gz, PLANES - 1, grecv_sem.at[0])

    def spread(o, c):
        in_plane_copy(o, gz, grecv, gsend_sem.at[1], grecv_sem.at[1]).start()
        return c

    lax.fori_loop(1, plane, spread, 0)
    grecv[my_in] = gz[...]
    send_rows(plane, ep_n)

    def load_block(pos, c):
        zt, it = peer(pos)
        src = zt * plane + it
        pltpu.make_async_copy(hg_in.at[src], hgv.at[pos], load_sem.at[3]).start()
        pltpu.make_async_copy(hu_in.at[src], huv.at[pos], load_sem.at[4]).start()
        pltpu.make_async_copy(y_in.at[src], yv.at[pos], load_sem.at[5]).start()
        pltpu.make_async_copy(x_in.at[src], xv.at[pos], load_sem.at[6]).start()
        return c

    lax.fori_loop(0, ep_n, load_block, 0)

    def wait_chunk(ci, buf, sem):
        @pl.when(ci > 0)
        def _():
            wait_bytes(buf, plane, sem)

        @pl.when(ci == 0)
        def _():
            wait_bytes(buf, plane - 1, sem)

    for i in (0, 1, 2):
        loads[i].wait()
        wcopies[i].wait()
    wait_bytes(hgv, ep_n, load_sem.at[3])
    wait_bytes(huv, ep_n, load_sem.at[4])
    wait_bytes(yv, ep_n, load_sem.at[5])
    wait_bytes(grecv, plane - 1, grecv_sem.at[1])

    lane_c = lax.broadcasted_iota(jnp.int32, (plane, cap, lanes), 2)
    sub_c = lax.broadcasted_iota(jnp.int32, (plane, cap, lanes), 1)
    mine = lane_c == my_in * cap + sub_c

    def chunk(ci, c):
        wait_chunk(ci, recv, frecv_sem.at[ci])
        rows = pl.ds(ci * rows_chunk, rows_chunk)
        blocks = pl.ds(ci * plane, plane)
        places = [peer(ci * plane + i) for i in range(plane)]
        dy = recv[blocks].astype(F32).reshape(rows_chunk, width)
        gate3 = jnp.where(mine, jnp.broadcast_to(jnp.stack([grecv[it, zt] for zt, it in places]), (plane, cap, lanes)), 0.0)
        gate = jnp.sum(gate3, axis=2, keepdims=True).reshape(rows_chunk, 1)
        g = (dy * gate).astype(BF16)
        gv[rows] = g
        val = jnp.sum(dy * yv[blocks].astype(F32).reshape(rows_chunk, width), axis=1, keepdims=True).reshape(plane, cap, 1)
        spread_val = jnp.sum(jnp.where(mine, val, 0.0), axis=1, keepdims=True)
        for i, (zt, it) in enumerate(places):
            vs[it, zt] = spread_val[i]

        @pl.when(ci == PLANES - 1)
        def _():
            def gather_back(o, cc):
                in_plane_copy(o, vs, vr, vsend_sem.at[0], vrecv_sem.at[0]).start()
                return cc

            lax.fori_loop(1, plane, gather_back, 0)

        da = lax.dot_general(g, wd[...], NT, preferred_element_type=F32)
        h1 = hgv[blocks].astype(F32).reshape(rows_chunk, hidden)
        h3 = huv[blocks].astype(F32).reshape(rows_chunk, hidden)
        sg = jax.nn.sigmoid(h1)
        silu = h1 * sg
        av[rows] = jnp.where(gate > 0.0, silu * h3, 0.0).astype(BF16)
        dhv[rows, pl.ds(0, hidden)] = (da * h3 * sg * (1.0 + h1 * (1.0 - sg))).astype(BF16)
        dhv[rows, pl.ds(hidden, hidden)] = (da * silu).astype(BF16)
        dx = lax.dot_general(dhv[rows], wgu[...], NT, preferred_element_type=F32)
        dxs[blocks] = dx.reshape(plane, cap, width).astype(BF16)

        def back_one(o, cc):
            pos = ci * plane + o

            @pl.when(pos > 0)
            def _():
                row_copy(dxs, dxr, pos, bsend_sem, brecv_sem).start()

            return cc

        lax.fori_loop(0, plane, back_one, 0)
        return c

    lax.fori_loop(0, PLANES, chunk, 0)
    dxr[0] = dxs[0]
    vr[my_in] = vs[my_in]

    wait_bytes(xv, ep_n, load_sem.at[6])

    def in_grads(base, to_g, to_u):
        tile = 256 if half_d % 256 == 0 else half_d

        def step(i, c):
            cols = pl.ds(pl.multiple_of(base + i * tile, tile), tile)
            xt = xv[:, :, cols].astype(F32).reshape(ep_n * cap, tile).astype(BF16)
            r = lax.dot_general(xt, dhv[...], TN, preferred_element_type=F32)
            to_g[pl.ds(i * tile, tile)] = r[:, :hidden]
            to_u[pl.ds(i * tile, tile)] = r[:, hidden:]
            return c

        lax.fori_loop(0, half_d // tile, step, 0)

    def out_grads(base, to_d):
        cols = pl.ds(pl.multiple_of(base, half_f), half_f)
        to_d[...] = lax.dot_general(av[:, cols], gv[...], TN, preferred_element_type=F32)

    in_grads(other * half_d, pg, pu)
    pcopies = [partner_copy(pg, rg, 0, psend_sem, precv_sem), partner_copy(pu, ru, 1, psend_sem, precv_sem)]
    pcopies[0].start()
    pcopies[1].start()
    out_grads(other * half_f, pd)
    pcopies.append(partner_copy(pd, rd, 2, psend_sem, precv_sem))
    pcopies[2].start()
    in_grads(q * half_d, og, ou)
    wait_bytes(vr, plane - 1, vrecv_sem.at[0])
    total = jnp.sum(vr[...], axis=0)
    vsum[...] = total
    back4[my_plane] = vsum[my_plane]
    out_grads(q * half_f, od)
    for dz in range(1, PLANES):
        line_copy(dz, vsum, back4, vsend_sem.at[1], vrecv_sem.at[1]).start()
    for i, (mine_ref, got) in enumerate(((og, rg), (ou, ru), (od, rd))):
        pcopies[i].wait()
        mine_ref[...] += got[...]

    wait_bytes(back4, PLANES - 1, vrecv_sem.at[1])
    acc = jnp.zeros((tok_n, width), F32)
    vals = [jnp.zeros((lanes, tok_n), F32) for _ in range(top)]
    for zp in range(PLANES):
        wait_bytes(dxr, plane - 1 if zp == 0 else plane, brecv_sem.at[zp])
        blocks = pl.ds(zp * plane, plane)
        part = dxr[blocks].astype(F32).reshape(rows_chunk, width).astype(BF16)
        acc = acc + lax.dot_general(onehot[zp], part, TN, preferred_element_type=F32)
        back = jnp.sum(jnp.where(diag, back4[zp], 0.0), axis=1, keepdims=True)
        for j in range(top):
            hit = slot_s == dest[j:j + 1, :] - zp * lanes
            vals[j] = jnp.where(hit, back, vals[j])
    gx[...] = acc.astype(BF16)
    for j in range(top):
        gg[j:j + 1, :] = jnp.sum(vals[j], axis=0, keepdims=True)

    wait_bytes(send, ep_n - 1, fsend_sem)
    wait_bytes(gz, PLANES - 1, gsend_sem.at[0])
    wait_bytes(grecv, plane - 1, gsend_sem.at[1])
    wait_bytes(dxs, ep_n - 1, bsend_sem)
    wait_bytes(vr, plane - 1, vsend_sem.at[0])
    wait_bytes(back4, PLANES - 1, vsend_sem.at[1])


def write_kernel(*refs):
    n = len(refs) // 2
    sem = refs[-1]
    copies = [pltpu.make_async_copy(refs[i], refs[n + i], sem.at[i]) for i in range(n)]
    for cp in copies:
        cp.start()
    for cp in copies:
        cp.wait()


def solution(mesh):
    ep_n = mesh.shape['ep']
    tok_spec = P(('fsdp', 'ep'), None)
    row_spec = P('ep', 'fsdp', None)

    def local_backward(grad_out, expert_idx, slot_pos, gates, x_disp, h_gate, h_up, y_disp, w_gate, w_down, w_up):
        tok_n, top = expert_idx.shape
        _, rows, width = x_disp.shape
        hidden = h_gate.shape[2]
        cap = rows // ep_n
        plane = ep_n // PLANES
        ysz = 4 if plane == 16 else 2
        xsz = plane // ysz
        lanes = plane * cap
        half_d, half_f = width // 2, hidden // 2
        cfg = (ep_n, top, tok_n, width, hidden, cap, ysz, xsz)
        vmem = pl.BlockSpec(memory_space=pltpu.VMEM)
        hbm = pl.BlockSpec(memory_space=pltpu.HBM)
        dma = pltpu.SemaphoreType.DMA
        rows_buf = pltpu.VMEM((ep_n, cap, width), BF16)
        line_buf = pltpu.VMEM((PLANES, 1, lanes), F32)
        gate_buf = pltpu.VMEM((plane, PLANES, 1, lanes), F32)
        in_part = pltpu.VMEM((half_d, hidden), F32)
        out_part = pltpu.VMEM((half_f, width), F32)
        results = [
            jax.ShapeDtypeStruct((tok_n, width), BF16),
            jax.ShapeDtypeStruct((top, tok_n), F32),
            jax.ShapeDtypeStruct((half_d, hidden), F32),
            jax.ShapeDtypeStruct((half_f, width), F32),
            jax.ShapeDtypeStruct((half_d, hidden), F32),
        ]
        outs = pl.pallas_call(
            functools.partial(layer_kernel, cfg),
            out_shape=results,
            in_specs=[hbm] * 11,
            out_specs=[vmem] * 5,
            scratch_shapes=[
                pltpu.VMEM((tok_n, width), BF16), pltpu.VMEM((top, tok_n), jnp.int32), pltpu.VMEM((top, tok_n), jnp.int32),
                pltpu.VMEM((top, tok_n), F32), rows_buf, rows_buf, line_buf, line_buf, gate_buf, rows_buf, rows_buf, gate_buf, gate_buf, line_buf, line_buf,
                rows_buf, rows_buf, pltpu.VMEM((ep_n, cap, hidden), BF16), pltpu.VMEM((ep_n, cap, hidden), BF16),
                pltpu.VMEM((width, 2 * hidden), BF16), pltpu.VMEM((hidden, width), BF16),
                pltpu.VMEM((PLANES, lanes, tok_n), BF16),
                pltpu.VMEM((rows, width), BF16), pltpu.VMEM((rows, hidden), BF16), pltpu.VMEM((rows, 2 * hidden), BF16),
                in_part, out_part, in_part, in_part, out_part, in_part,
                dma((11,)), dma((3,)), dma((3,)), dma, dma((PLANES,)), dma((2,)), dma((2,)),
                dma, dma((PLANES,)), dma((2,)), dma((2,)), dma((3,)), dma((3,)),
            ],
            compiler_params=pltpu.CompilerParams(collective_id=0, has_side_effects=True, vmem_limit_bytes=44 * 1024 * 1024),
            name='layer',
        )(*[pltpu.with_memory_space_constraint(v, pltpu.HBM) for v in (grad_out, expert_idx.T, slot_pos.T, gates.T, *[v.reshape(ep_n, cap, v.shape[2]) for v in (x_disp, h_gate, h_up, y_disp)], w_gate[0], w_down[0], w_up[0])])
        gx, gg, dwg, dwd, dwu = pl.pallas_call(
            write_kernel,
            out_shape=results,
            in_specs=[vmem] * 5,
            out_specs=[hbm] * 5,
            scratch_shapes=[dma((5,))],
            compiler_params=pltpu.CompilerParams(vmem_limit_bytes=8 * 1024 * 1024),
            name='write',
        )(*outs)
        return gx, gg.T, dwg[None], dwd[None], dwu[None]

    return jax.shard_map(local_backward, mesh=mesh, in_specs=(tok_spec, tok_spec, tok_spec, tok_spec, row_spec, row_spec, row_spec, row_spec, row_spec, row_spec, row_spec), out_specs=(tok_spec, tok_spec, row_spec, row_spec, row_spec), check_vma=False)
```

```python
import functools

import jax
import jax.numpy as jnp
from jax import lax
from jax.experimental import pallas as pl
from jax.experimental.pallas import tpu as pltpu
from jax.sharding import PartitionSpec as P

MESH = pl.DeviceIdType.MESH
F32 = jnp.float32
BF16 = jnp.bfloat16
PLANES = 4
NT = (((1,), (1,)), ((), ()))
TN = (((0,), (0,)), ((), ()))


def layer_kernel(cfg, go_in, eidx_in, slot_in, gates_in, x_in, hg_in, hu_in, y_in, wg_in, wd_in, wu_in,
                 gx, gg, og, od, ou,
                 go, eidx, slot, gates, send, recv, gsend, gz, grecv, dxs, dxr, vs, vr, vsum, back4,
                 xv, yv, hgv, huv, wgu, wd, onehot, gv, av, dhv,
                 pg, pd, pu, rg, rd, ru,
                 load_sem, wsend_sem, wrecv_sem, fsend_sem, frecv_sem, gsend_sem, grecv_sem,
                 bsend_sem, brecv_sem, vsend_sem, vrecv_sem, psend_sem, precv_sem):
    ep_n, top, tok_n, width, hidden, cap, ysz, xsz = cfg
    plane = ep_n // PLANES
    lanes = plane * cap
    rows_chunk = plane * cap
    half_d, half_f = width // 2, hidden // 2
    q = lax.axis_index('fsdp')
    me = lax.axis_index('ep')
    other = 1 - q
    my_plane = me // plane
    my_in = lax.rem(me, plane)

    my_y, my_x = my_in // xsz, lax.rem(my_in, xsz)

    def walk(c, k, n):
        return lax.rem(c + (1 - 2 * lax.rem(c, 2)) * k + n, n)

    def peer_in(o):
        return walk(my_y, o // xsz, ysz) * xsz + walk(my_x, lax.rem(o, xsz), xsz)

    def peer(pos):
        o = lax.rem(pos, plane)
        dz = lax.rem(o // xsz + lax.rem(o, xsz) + pos // plane, PLANES)
        return walk(my_plane, dz, PLANES), peer_in(o)

    barrier = pltpu.get_barrier_semaphore()

    def announce(o, c):
        pl.semaphore_signal(barrier, inc=1, device_id=(q, lax.rem(me + o, ep_n)), device_id_type=MESH)
        return c

    lax.fori_loop(1, ep_n, announce, 0)
    pl.semaphore_signal(barrier, inc=1, device_id=(other, me), device_id_type=MESH)

    small = [
        pltpu.make_async_copy(src, dst, load_sem.at[7 + i])
        for i, (src, dst) in enumerate(((eidx_in, eidx), (slot_in, slot), (gates_in, gates), (go_in, go)))
    ]
    for cp in small:
        cp.start()
    loads = [
        pltpu.make_async_copy(wd_in, wd.at[pl.ds(q * half_f, half_f)], load_sem.at[0]),
        pltpu.make_async_copy(wg_in, wgu.at[pl.ds(q * half_d, half_d), pl.ds(0, hidden)], load_sem.at[1]),
        pltpu.make_async_copy(wu_in, wgu.at[pl.ds(q * half_d, half_d), pl.ds(hidden, hidden)], load_sem.at[2]),
    ]
    for cp in loads:
        cp.start()

    for cp in small:
        cp.wait()
    kept = slot[...] >= 0
    dest = jnp.where(kept, eidx[...] * cap + slot[...], ep_n * cap)

    def steps(place, c, n):
        return ((1 - 2 * lax.rem(c, 2)) * (place - c) + 2 * n) & (n - 1)

    place_in = eidx[...] & (plane - 1)
    dz = steps(eidx[...] >> (plane.bit_length() - 1), my_plane, PLANES)
    dy = steps(place_in >> (xsz.bit_length() - 1), my_y, ysz)
    dx = steps(place_in & (xsz - 1), my_x, xsz)
    pos_of = ((dz - dy - dx + 2 * PLANES) & (PLANES - 1)) * plane + dy * xsz + dx
    dest_pos = jnp.where(kept, pos_of * cap + slot[...], ep_n * cap)
    slot_s = lax.broadcasted_iota(jnp.int32, (lanes, tok_n), 0)
    diag = lax.broadcasted_iota(jnp.int32, (lanes, lanes), 0) == lax.broadcasted_iota(jnp.int32, (lanes, lanes), 1)
    for k in range(PLANES):
        hot = jnp.zeros((lanes, tok_n), F32)
        gate = jnp.zeros((lanes, tok_n), F32)
        for j in range(top):
            hot = jnp.where(slot_s == dest_pos[j:j + 1, :] - k * lanes, 1.0, hot)
            gate = jnp.where(slot_s == dest[j:j + 1, :] - k * lanes, gates[j:j + 1, :], gate)
        hot = hot.astype(BF16)
        onehot[k] = hot
        gate_col = jnp.sum(gate, axis=1, keepdims=True)
        gsend[k] = jnp.sum(jnp.where(diag, gate_col, 0.0), axis=0, keepdims=True)
        picked = jnp.dot(hot, go[...], preferred_element_type=F32)
        send[pl.ds(k * plane, plane)] = picked.reshape(plane, cap, width).astype(BF16)

    def load_block(pos, c):
        zt, it = peer(pos)
        src = zt * plane + it
        pltpu.make_async_copy(hg_in.at[src], hgv.at[pos], load_sem.at[3]).start()
        pltpu.make_async_copy(hu_in.at[src], huv.at[pos], load_sem.at[4]).start()
        pltpu.make_async_copy(y_in.at[src], yv.at[pos], load_sem.at[5]).start()
        pltpu.make_async_copy(x_in.at[src], xv.at[pos], load_sem.at[6]).start()
        return c

    lax.fori_loop(0, ep_n, load_block, 0)

    pl.semaphore_wait(barrier, ep_n)

    def partner_copy(src, dst, i, ssem, rsem):
        return pltpu.make_async_remote_copy(src_ref=src, dst_ref=dst, send_sem=ssem.at[i], recv_sem=rsem.at[i],
                                            device_id=(other, me), device_id_type=MESH)

    wcopies = [
        partner_copy(wd_in, wd.at[pl.ds(q * half_f, half_f)], 0, wsend_sem, wrecv_sem),
        partner_copy(wg_in, wgu.at[pl.ds(q * half_d, half_d), pl.ds(0, hidden)], 1, wsend_sem, wrecv_sem),
        partner_copy(wu_in, wgu.at[pl.ds(q * half_d, half_d), pl.ds(hidden, hidden)], 2, wsend_sem, wrecv_sem),
    ]

    def row_copy(src, dst, pos, ssem, rsem):
        zt, it = peer(pos)
        return pltpu.make_async_remote_copy(src_ref=src.at[pos], dst_ref=dst.at[pos], send_sem=ssem,
                                            recv_sem=rsem.at[pos // plane], device_id=(q, zt * plane + it), device_id_type=MESH)

    def line_copy(dz, src, dst, ssem, rsem):
        zt = lax.rem(my_plane + dz, PLANES)
        return pltpu.make_async_remote_copy(src_ref=src.at[zt], dst_ref=dst.at[my_plane], send_sem=ssem, recv_sem=rsem,
                                            device_id=(q, zt * plane + my_in), device_id_type=MESH)

    def in_plane_copy(o, src, dst, ssem, rsem):
        to = peer_in(o)
        part = src if len(src.shape) == 3 else src.at[to]
        return pltpu.make_async_remote_copy(src_ref=part, dst_ref=dst.at[my_in], send_sem=ssem, recv_sem=rsem,
                                            device_id=(q, my_plane * plane + to), device_id_type=MESH)

    def wait_bytes(buf, n, sem):
        part = buf.at[pl.ds(0, n)]
        pltpu.make_async_copy(part, part, sem).wait()

    def send_rows(lo, hi):
        def send_one(pos, c):
            row_copy(send, recv, pos, fsend_sem, frecv_sem).start()
            return c

        lax.fori_loop(lo, hi, send_one, 0)

    for dz in range(1, PLANES):
        line_copy(dz, gsend, gz, gsend_sem.at[0], grecv_sem.at[0]).start()
    send_rows(1, plane)
    for cp in wcopies:
        cp.start()
    send_rows(plane, 2 * plane)
    recv[0] = send[0]
    gz[my_plane] = gsend[my_plane]
    wait_bytes(gz, PLANES - 1, grecv_sem.at[0])

    def spread(o, c):
        in_plane_copy(o, gz, grecv, gsend_sem.at[1], grecv_sem.at[1]).start()
        return c

    lax.fori_loop(1, plane, spread, 0)
    grecv[my_in] = gz[...]
    send_rows(2 * plane, ep_n)


    def wait_chunk(ci, buf, sem):
        @pl.when(ci > 0)
        def _():
            wait_bytes(buf, plane, sem)

        @pl.when(ci == 0)
        def _():
            wait_bytes(buf, plane - 1, sem)

    for i in (0, 1, 2):
        loads[i].wait()
        wcopies[i].wait()
    wait_bytes(hgv, ep_n, load_sem.at[3])
    wait_bytes(huv, ep_n, load_sem.at[4])
    wait_bytes(yv, ep_n, load_sem.at[5])
    wait_bytes(grecv, plane - 1, grecv_sem.at[1])

    lane_c = lax.broadcasted_iota(jnp.int32, (plane, cap, lanes), 2)
    sub_c = lax.broadcasted_iota(jnp.int32, (plane, cap, lanes), 1)
    mine = lane_c == my_in * cap + sub_c

    def chunk(ci, c):
        wait_chunk(ci, recv, frecv_sem.at[ci])
        rows = pl.ds(ci * rows_chunk, rows_chunk)
        blocks = pl.ds(ci * plane, plane)
        places = [peer(ci * plane + i) for i in range(plane)]
        dy = recv[blocks].astype(F32).reshape(rows_chunk, width)
        gate3 = jnp.where(mine, jnp.broadcast_to(jnp.stack([grecv[it, zt] for zt, it in places]), (plane, cap, lanes)), 0.0)
        gate = jnp.sum(gate3, axis=2, keepdims=True).reshape(rows_chunk, 1)
        g = (dy * gate).astype(BF16)
        gv[rows] = g
        val = jnp.sum(dy * yv[blocks].astype(F32).reshape(rows_chunk, width), axis=1, keepdims=True).reshape(plane, cap, 1)
        spread_val = jnp.sum(jnp.where(mine, val, 0.0), axis=1, keepdims=True)
        for i, (zt, it) in enumerate(places):
            vs[it, zt] = spread_val[i]

        @pl.when(ci == PLANES - 1)
        def _():
            def gather_back(o, cc):
                in_plane_copy(o, vs, vr, vsend_sem.at[0], vrecv_sem.at[0]).start()
                return cc

            lax.fori_loop(1, plane, gather_back, 0)

        da = lax.dot_general(g, wd[...], NT, preferred_element_type=F32)
        h1 = hgv[blocks].astype(F32).reshape(rows_chunk, hidden)
        h3 = huv[blocks].astype(F32).reshape(rows_chunk, hidden)
        sg = jax.nn.sigmoid(h1)
        silu = h1 * sg
        av[rows] = jnp.where(gate > 0.0, silu * h3, 0.0).astype(BF16)
        dhv[rows, pl.ds(0, hidden)] = (da * h3 * sg * (1.0 + h1 * (1.0 - sg))).astype(BF16)
        dhv[rows, pl.ds(hidden, hidden)] = (da * silu).astype(BF16)
        dx = lax.dot_general(dhv[rows], wgu[...], NT, preferred_element_type=F32)
        dxs[blocks] = dx.reshape(plane, cap, width).astype(BF16)

        def back_one(o, cc):
            pos = ci * plane + o

            @pl.when(pos > 0)
            def _():
                row_copy(dxs, dxr, pos, bsend_sem, brecv_sem).start()

            return cc

        lax.fori_loop(0, plane, back_one, 0)
        return c

    lax.fori_loop(0, PLANES, chunk, 0)
    dxr[0] = dxs[0]
    vr[my_in] = vs[my_in]

    wait_bytes(xv, ep_n, load_sem.at[6])

    def in_grads(base, to_g, to_u):
        tile = 256 if half_d % 256 == 0 else half_d

        def step(i, c):
            cols = pl.ds(pl.multiple_of(base + i * tile, tile), tile)
            xt = xv[:, :, cols].astype(F32).reshape(ep_n * cap, tile).astype(BF16)
            r = lax.dot_general(xt, dhv[...], TN, preferred_element_type=F32)
            to_g[pl.ds(i * tile, tile)] = r[:, :hidden]
            to_u[pl.ds(i * tile, tile)] = r[:, hidden:]
            return c

        lax.fori_loop(0, half_d // tile, step, 0)

    def out_grads(base, to_d):
        cols = pl.ds(pl.multiple_of(base, half_f), half_f)
        to_d[...] = lax.dot_general(av[:, cols], gv[...], TN, preferred_element_type=F32)

    in_grads(other * half_d, pg, pu)
    pcopies = [partner_copy(pg, rg, 0, psend_sem, precv_sem), partner_copy(pu, ru, 1, psend_sem, precv_sem)]
    pcopies[0].start()
    pcopies[1].start()
    out_grads(other * half_f, pd)
    pcopies.append(partner_copy(pd, rd, 2, psend_sem, precv_sem))
    pcopies[2].start()
    in_grads(q * half_d, og, ou)
    wait_bytes(vr, plane - 1, vrecv_sem.at[0])
    total = jnp.sum(vr[...], axis=0)
    vsum[...] = total
    back4[my_plane] = vsum[my_plane]
    out_grads(q * half_f, od)
    for dz in range(1, PLANES):
        line_copy(dz, vsum, back4, vsend_sem.at[1], vrecv_sem.at[1]).start()
    for i, (mine_ref, got) in enumerate(((og, rg), (ou, ru), (od, rd))):
        pcopies[i].wait()
        mine_ref[...] += got[...]

    wait_bytes(back4, PLANES - 1, vrecv_sem.at[1])
    acc = jnp.zeros((tok_n, width), F32)
    vals = [jnp.zeros((lanes, tok_n), F32) for _ in range(top)]
    for zp in range(PLANES):
        wait_bytes(dxr, plane - 1 if zp == 0 else plane, brecv_sem.at[zp])
        blocks = pl.ds(zp * plane, plane)
        part = dxr[blocks].astype(F32).reshape(rows_chunk, width).astype(BF16)
        acc = acc + lax.dot_general(onehot[zp], part, TN, preferred_element_type=F32)
        back = jnp.sum(jnp.where(diag, back4[zp], 0.0), axis=1, keepdims=True)
        for j in range(top):
            hit = slot_s == dest[j:j + 1, :] - zp * lanes
            vals[j] = jnp.where(hit, back, vals[j])
    gx[...] = acc.astype(BF16)
    for j in range(top):
        gg[j:j + 1, :] = jnp.sum(vals[j], axis=0, keepdims=True)

    wait_bytes(send, ep_n - 1, fsend_sem)
    wait_bytes(gz, PLANES - 1, gsend_sem.at[0])
    wait_bytes(grecv, plane - 1, gsend_sem.at[1])
    wait_bytes(dxs, ep_n - 1, bsend_sem)
    wait_bytes(vr, plane - 1, vsend_sem.at[0])
    wait_bytes(back4, PLANES - 1, vsend_sem.at[1])


def write_kernel(*refs):
    n = len(refs) // 2
    sem = refs[-1]
    copies = [pltpu.make_async_copy(refs[i], refs[n + i], sem.at[i]) for i in range(n)]
    for cp in copies:
        cp.start()
    for cp in copies:
        cp.wait()


def solution(mesh):
    ep_n = mesh.shape['ep']
    tok_spec = P(('fsdp', 'ep'), None)
    row_spec = P('ep', 'fsdp', None)

    def local_backward(grad_out, expert_idx, slot_pos, gates, x_disp, h_gate, h_up, y_disp, w_gate, w_down, w_up):
        tok_n, top = expert_idx.shape
        _, rows, width = x_disp.shape
        hidden = h_gate.shape[2]
        cap = rows // ep_n
        plane = ep_n // PLANES
        ysz = 4 if plane == 16 else 2
        xsz = plane // ysz
        lanes = plane * cap
        half_d, half_f = width // 2, hidden // 2
        cfg = (ep_n, top, tok_n, width, hidden, cap, ysz, xsz)
        vmem = pl.BlockSpec(memory_space=pltpu.VMEM)
        hbm = pl.BlockSpec(memory_space=pltpu.HBM)
        dma = pltpu.SemaphoreType.DMA
        rows_buf = pltpu.VMEM((ep_n, cap, width), BF16)
        line_buf = pltpu.VMEM((PLANES, 1, lanes), F32)
        gate_buf = pltpu.VMEM((plane, PLANES, 1, lanes), F32)
        in_part = pltpu.VMEM((half_d, hidden), F32)
        out_part = pltpu.VMEM((half_f, width), F32)
        results = [
            jax.ShapeDtypeStruct((tok_n, width), BF16),
            jax.ShapeDtypeStruct((top, tok_n), F32),
            jax.ShapeDtypeStruct((half_d, hidden), F32),
            jax.ShapeDtypeStruct((half_f, width), F32),
            jax.ShapeDtypeStruct((half_d, hidden), F32),
        ]
        outs = pl.pallas_call(
            functools.partial(layer_kernel, cfg),
            out_shape=results,
            in_specs=[hbm] * 11,
            out_specs=[vmem] * 5,
            scratch_shapes=[
                pltpu.VMEM((tok_n, width), BF16), pltpu.VMEM((top, tok_n), jnp.int32), pltpu.VMEM((top, tok_n), jnp.int32),
                pltpu.VMEM((top, tok_n), F32), rows_buf, rows_buf, line_buf, line_buf, gate_buf, rows_buf, rows_buf, gate_buf, gate_buf, line_buf, line_buf,
                rows_buf, rows_buf, pltpu.VMEM((ep_n, cap, hidden), BF16), pltpu.VMEM((ep_n, cap, hidden), BF16),
                pltpu.VMEM((width, 2 * hidden), BF16), pltpu.VMEM((hidden, width), BF16),
                pltpu.VMEM((PLANES, lanes, tok_n), BF16),
                pltpu.VMEM((rows, width), BF16), pltpu.VMEM((rows, hidden), BF16), pltpu.VMEM((rows, 2 * hidden), BF16),
                in_part, out_part, in_part, in_part, out_part, in_part,
                dma((11,)), dma((3,)), dma((3,)), dma, dma((PLANES,)), dma((2,)), dma((2,)),
                dma, dma((PLANES,)), dma((2,)), dma((2,)), dma((3,)), dma((3,)),
            ],
            compiler_params=pltpu.CompilerParams(collective_id=0, has_side_effects=True, vmem_limit_bytes=44 * 1024 * 1024),
            name='layer',
        )(*[pltpu.with_memory_space_constraint(v, pltpu.HBM) for v in (grad_out, expert_idx.T, slot_pos.T, gates.T, *[v.reshape(ep_n, cap, v.shape[2]) for v in (x_disp, h_gate, h_up, y_disp)], w_gate[0], w_down[0], w_up[0])])
        gx, gg, dwg, dwd, dwu = pl.pallas_call(
            write_kernel,
            out_shape=results,
            in_specs=[vmem] * 5,
            out_specs=[hbm] * 5,
            scratch_shapes=[dma((5,))],
            compiler_params=pltpu.CompilerParams(vmem_limit_bytes=8 * 1024 * 1024),
            name='write',
        )(*outs)
        return gx, gg.T, dwg[None], dwd[None], dwu[None]

    return jax.shard_map(local_backward, mesh=mesh, in_specs=(tok_spec, tok_spec, tok_spec, tok_spec, row_spec, row_spec, row_spec, row_spec, row_spec, row_spec, row_spec), out_specs=(tok_spec, tok_spec, row_spec, row_spec, row_spec), check_vma=False)
```

```python
import functools

import jax
import jax.numpy as jnp
from jax import lax
from jax.experimental import pallas as pl
from jax.experimental.pallas import tpu as pltpu
from jax.sharding import PartitionSpec as P

MESH = pl.DeviceIdType.MESH
F32 = jnp.float32
BF16 = jnp.bfloat16
PLANES = 4
NT = (((1,), (1,)), ((), ()))
TN = (((0,), (0,)), ((), ()))


def far_first(ysz, xsz):
    left = [(dz, dy, dx) for dz in range(PLANES) for dy in range(ysz) for dx in range(xsz)]
    sizes = (PLANES, ysz, xsz)

    def hops(o):
        return sum(min(k, n - k) for k, n in zip(o, sizes))

    load, order = [0] * 6, []

    def added(o):
        new = list(load)
        for d, (k, n) in enumerate(zip(o, sizes)):
            if 2 * k <= n:
                new[2 * d] += k
            if 2 * k >= n and k:
                new[2 * d + 1] += n - k
        return new

    while left:
        most = max(hops(o) for o in left)
        best = min((o for o in left if hops(o) == most), key=lambda o: (max(added(o)), sum(v * v for v in added(o)), o))
        load = added(best)
        order.append(best)
        left.remove(best)
    return order


def layer_kernel(cfg, go_in, eidx_in, slot_in, gates_in, x_in, hg_in, hu_in, y_in, wg_in, wd_in, wu_in,
                 gx, gg, og, od, ou,
                 go, eidx, slot, gates, send, recv, gsend, gz, grecv, dxs, dxr, vs, vr, vsum, back4,
                 xv, yv, hgv, huv, wgu, wd, onehot, gv, av, dhv,
                 pg, pd, pu, rg, rd, ru,
                 load_sem, wsend_sem, wrecv_sem, fsend_sem, frecv_sem, gsend_sem, grecv_sem,
                 bsend_sem, brecv_sem, vsend_sem, vrecv_sem, psend_sem, precv_sem):
    ep_n, top, tok_n, width, hidden, cap, ysz, xsz = cfg
    plane = ep_n // PLANES
    lanes = plane * cap
    rows_chunk = plane * cap
    half_d, half_f = width // 2, hidden // 2
    q = lax.axis_index('fsdp')
    me = lax.axis_index('ep')
    other = 1 - q
    my_plane = me // plane
    my_in = lax.rem(me, plane)

    my_y, my_x = my_in // xsz, lax.rem(my_in, xsz)

    def walk(c, k, n):
        return lax.rem(c + (1 - 2 * lax.rem(c, 2)) * k + n, n)

    def peer_in(o):
        return walk(my_y, o // xsz, ysz) * xsz + walk(my_x, lax.rem(o, xsz), xsz)

    offsets = far_first(ysz, xsz)
    own = ep_n - 1

    def peer(pos):
        dz, dy, dx = offsets[pos]
        return walk(my_plane, dz, PLANES), walk(my_y, dy, ysz) * xsz + walk(my_x, dx, xsz)

    barrier = pltpu.get_barrier_semaphore()

    def announce(o, c):
        pl.semaphore_signal(barrier, inc=1, device_id=(q, lax.rem(me + o, ep_n)), device_id_type=MESH)
        return c

    lax.fori_loop(1, ep_n, announce, 0)
    pl.semaphore_signal(barrier, inc=1, device_id=(other, me), device_id_type=MESH)

    small = [
        pltpu.make_async_copy(src, dst, load_sem.at[7 + i])
        for i, (src, dst) in enumerate(((eidx_in, eidx), (slot_in, slot), (gates_in, gates), (go_in, go)))
    ]
    for cp in small:
        cp.start()
    loads = [
        pltpu.make_async_copy(wd_in, wd.at[pl.ds(q * half_f, half_f)], load_sem.at[0]),
        pltpu.make_async_copy(wg_in, wgu.at[pl.ds(q * half_d, half_d), pl.ds(0, hidden)], load_sem.at[1]),
        pltpu.make_async_copy(wu_in, wgu.at[pl.ds(q * half_d, half_d), pl.ds(hidden, hidden)], load_sem.at[2]),
    ]
    for cp in loads:
        cp.start()

    for cp in small:
        cp.wait()
    kept = slot[...] >= 0
    dest = jnp.where(kept, eidx[...] * cap + slot[...], ep_n * cap)

    def steps(place, c, n):
        return ((1 - 2 * lax.rem(c, 2)) * (place - c) + 2 * n) & (n - 1)

    place_in = eidx[...] & (plane - 1)
    dz = steps(eidx[...] >> (plane.bit_length() - 1), my_plane, PLANES)
    dy = steps(place_in >> (xsz.bit_length() - 1), my_y, ysz)
    dx = steps(place_in & (xsz - 1), my_x, xsz)
    off = (dz * ysz + dy) * xsz + dx
    pos_of = jnp.zeros_like(off)
    for pos, (kz, ky, kx) in enumerate(offsets):
        pos_of = jnp.where(off == (kz * ysz + ky) * xsz + kx, pos, pos_of)
    dest_pos = jnp.where(kept, pos_of * cap + slot[...], ep_n * cap)
    slot_s = lax.broadcasted_iota(jnp.int32, (lanes, tok_n), 0)
    diag = lax.broadcasted_iota(jnp.int32, (lanes, lanes), 0) == lax.broadcasted_iota(jnp.int32, (lanes, lanes), 1)
    for k in range(PLANES):
        hot = jnp.zeros((lanes, tok_n), F32)
        gate = jnp.zeros((lanes, tok_n), F32)
        for j in range(top):
            hot = jnp.where(slot_s == dest_pos[j:j + 1, :] - k * lanes, 1.0, hot)
            gate = jnp.where(slot_s == dest[j:j + 1, :] - k * lanes, gates[j:j + 1, :], gate)
        hot = hot.astype(BF16)
        onehot[k] = hot
        gate_col = jnp.sum(gate, axis=1, keepdims=True)
        gsend[k] = jnp.sum(jnp.where(diag, gate_col, 0.0), axis=0, keepdims=True)
        picked = jnp.dot(hot, go[...], preferred_element_type=F32)
        send[pl.ds(k * plane, plane)] = picked.reshape(plane, cap, width).astype(BF16)

    pl.semaphore_wait(barrier, ep_n)

    def partner_copy(src, dst, i, ssem, rsem):
        return pltpu.make_async_remote_copy(src_ref=src, dst_ref=dst, send_sem=ssem.at[i], recv_sem=rsem.at[i],
                                            device_id=(other, me), device_id_type=MESH)

    wcopies = [
        partner_copy(wd_in, wd.at[pl.ds(q * half_f, half_f)], 0, wsend_sem, wrecv_sem),
        partner_copy(wg_in, wgu.at[pl.ds(q * half_d, half_d), pl.ds(0, hidden)], 1, wsend_sem, wrecv_sem),
        partner_copy(wu_in, wgu.at[pl.ds(q * half_d, half_d), pl.ds(hidden, hidden)], 2, wsend_sem, wrecv_sem),
    ]
    for cp in wcopies:
        cp.start()

    def row_copy(src, dst, pos, ssem, rsem):
        zt, it = peer(pos)
        return pltpu.make_async_remote_copy(src_ref=src.at[pos], dst_ref=dst.at[pos], send_sem=ssem,
                                            recv_sem=rsem.at[pos // plane], device_id=(q, zt * plane + it), device_id_type=MESH)

    def line_copy(dz, src, dst, ssem, rsem):
        zt = lax.rem(my_plane + dz, PLANES)
        return pltpu.make_async_remote_copy(src_ref=src.at[zt], dst_ref=dst.at[my_plane], send_sem=ssem, recv_sem=rsem,
                                            device_id=(q, zt * plane + my_in), device_id_type=MESH)

    def in_plane_copy(o, src, dst, ssem, rsem):
        to = peer_in(o)
        part = src if len(src.shape) == 3 else src.at[to]
        return pltpu.make_async_remote_copy(src_ref=part, dst_ref=dst.at[my_in], send_sem=ssem, recv_sem=rsem,
                                            device_id=(q, my_plane * plane + to), device_id_type=MESH)

    def wait_bytes(buf, n, sem):
        part = buf.at[pl.ds(0, n)]
        pltpu.make_async_copy(part, part, sem).wait()

    def send_rows(lo, hi):
        for pos in range(lo, hi):
            row_copy(send, recv, pos, fsend_sem, frecv_sem).start()

    for dz in range(1, PLANES):
        line_copy(dz, gsend, gz, gsend_sem.at[0], grecv_sem.at[0]).start()
    send_rows(0, plane)
    recv[own] = send[own]
    gz[my_plane] = gsend[my_plane]
    wait_bytes(gz, PLANES - 1, grecv_sem.at[0])

    def spread(o, c):
        in_plane_copy(o, gz, grecv, gsend_sem.at[1], grecv_sem.at[1]).start()
        return c

    lax.fori_loop(1, plane, spread, 0)
    grecv[my_in] = gz[...]
    send_rows(plane, own)

    for pos in range(ep_n):
        zt, it = peer(pos)
        src = zt * plane + it
        pltpu.make_async_copy(hg_in.at[src], hgv.at[pos], load_sem.at[3]).start()
        pltpu.make_async_copy(hu_in.at[src], huv.at[pos], load_sem.at[4]).start()
        pltpu.make_async_copy(y_in.at[src], yv.at[pos], load_sem.at[5]).start()
        pltpu.make_async_copy(x_in.at[src], xv.at[pos], load_sem.at[6]).start()

    def in_chunk(ci):
        return plane - 1 if ci == PLANES - 1 else plane

    for i in (0, 1, 2):
        loads[i].wait()
        wcopies[i].wait()
    wait_bytes(hgv, ep_n, load_sem.at[3])
    wait_bytes(huv, ep_n, load_sem.at[4])
    wait_bytes(yv, ep_n, load_sem.at[5])
    wait_bytes(grecv, plane - 1, grecv_sem.at[1])

    lane_c = lax.broadcasted_iota(jnp.int32, (plane, cap, lanes), 2)
    sub_c = lax.broadcasted_iota(jnp.int32, (plane, cap, lanes), 1)
    mine = lane_c == my_in * cap + sub_c

    def chunk(ci):
        wait_bytes(recv, in_chunk(ci), frecv_sem.at[ci])
        rows = pl.ds(ci * rows_chunk, rows_chunk)
        blocks = pl.ds(ci * plane, plane)
        places = [peer(ci * plane + i) for i in range(plane)]
        dy = recv[blocks].astype(F32).reshape(rows_chunk, width)
        gate3 = jnp.where(mine, jnp.broadcast_to(jnp.stack([grecv[it, zt] for zt, it in places]), (plane, cap, lanes)), 0.0)
        gate = jnp.sum(gate3, axis=2, keepdims=True).reshape(rows_chunk, 1)
        g = (dy * gate).astype(BF16)
        gv[rows] = g
        val = jnp.sum(dy * yv[blocks].astype(F32).reshape(rows_chunk, width), axis=1, keepdims=True).reshape(plane, cap, 1)
        spread_val = jnp.sum(jnp.where(mine, val, 0.0), axis=1, keepdims=True)
        for i, (zt, it) in enumerate(places):
            vs[it, zt] = spread_val[i]

        if ci == PLANES - 1:
            def gather_back(o, cc):
                in_plane_copy(o, vs, vr, vsend_sem.at[0], vrecv_sem.at[0]).start()
                return cc

            lax.fori_loop(1, plane, gather_back, 0)

        da = lax.dot_general(g, wd[...], NT, preferred_element_type=F32)
        h1 = hgv[blocks].astype(F32).reshape(rows_chunk, hidden)
        h3 = huv[blocks].astype(F32).reshape(rows_chunk, hidden)
        sg = jax.nn.sigmoid(h1)
        silu = h1 * sg
        av[rows] = jnp.where(gate > 0.0, silu * h3, 0.0).astype(BF16)
        dhv[rows, pl.ds(0, hidden)] = (da * h3 * sg * (1.0 + h1 * (1.0 - sg))).astype(BF16)
        dhv[rows, pl.ds(hidden, hidden)] = (da * silu).astype(BF16)
        dx = lax.dot_general(dhv[rows], wgu[...], NT, preferred_element_type=F32)
        dxs[blocks] = dx.reshape(plane, cap, width).astype(BF16)

        for i in range(in_chunk(ci)):
            row_copy(dxs, dxr, ci * plane + i, bsend_sem, brecv_sem).start()

    for ci in range(PLANES):
        chunk(ci)
    dxr[own] = dxs[own]
    vr[my_in] = vs[my_in]

    wait_bytes(xv, ep_n, load_sem.at[6])

    def in_grads(base, to_g, to_u):
        tile = 256 if half_d % 256 == 0 else half_d

        def step(i, c):
            cols = pl.ds(pl.multiple_of(base + i * tile, tile), tile)
            xt = xv[:, :, cols].astype(F32).reshape(ep_n * cap, tile).astype(BF16)
            r = lax.dot_general(xt, dhv[...], TN, preferred_element_type=F32)
            to_g[pl.ds(i * tile, tile)] = r[:, :hidden]
            to_u[pl.ds(i * tile, tile)] = r[:, hidden:]
            return c

        lax.fori_loop(0, half_d // tile, step, 0)

    def out_grads(base, to_d):
        cols = pl.ds(pl.multiple_of(base, half_f), half_f)
        to_d[...] = lax.dot_general(av[:, cols], gv[...], TN, preferred_element_type=F32)

    in_grads(other * half_d, pg, pu)
    pcopies = [partner_copy(pg, rg, 0, psend_sem, precv_sem), partner_copy(pu, ru, 1, psend_sem, precv_sem)]
    pcopies[0].start()
    pcopies[1].start()
    out_grads(other * half_f, pd)
    pcopies.append(partner_copy(pd, rd, 2, psend_sem, precv_sem))
    pcopies[2].start()
    in_grads(q * half_d, og, ou)
    wait_bytes(vr, plane - 1, vrecv_sem.at[0])
    total = jnp.sum(vr[...], axis=0)
    vsum[...] = total
    back4[my_plane] = vsum[my_plane]
    out_grads(q * half_f, od)
    for dz in range(1, PLANES):
        line_copy(dz, vsum, back4, vsend_sem.at[1], vrecv_sem.at[1]).start()
    for i, (mine_ref, got) in enumerate(((og, rg), (ou, ru), (od, rd))):
        pcopies[i].wait()
        mine_ref[...] += got[...]

    wait_bytes(back4, PLANES - 1, vrecv_sem.at[1])
    acc = jnp.zeros((tok_n, width), F32)
    vals = [jnp.zeros((lanes, tok_n), F32) for _ in range(top)]
    for zp in range(PLANES):
        wait_bytes(dxr, in_chunk(zp), brecv_sem.at[zp])
        blocks = pl.ds(zp * plane, plane)
        part = dxr[blocks].astype(F32).reshape(rows_chunk, width).astype(BF16)
        acc = acc + lax.dot_general(onehot[zp], part, TN, preferred_element_type=F32)
        back = jnp.sum(jnp.where(diag, back4[zp], 0.0), axis=1, keepdims=True)
        for j in range(top):
            hit = slot_s == dest[j:j + 1, :] - zp * lanes
            vals[j] = jnp.where(hit, back, vals[j])
    gx[...] = acc.astype(BF16)
    for j in range(top):
        gg[j:j + 1, :] = jnp.sum(vals[j], axis=0, keepdims=True)

    wait_bytes(send, ep_n - 1, fsend_sem)
    wait_bytes(gz, PLANES - 1, gsend_sem.at[0])
    wait_bytes(grecv, plane - 1, gsend_sem.at[1])
    wait_bytes(dxs, ep_n - 1, bsend_sem)
    wait_bytes(vr, plane - 1, vsend_sem.at[0])
    wait_bytes(back4, PLANES - 1, vsend_sem.at[1])


def write_kernel(*refs):
    n = len(refs) // 2
    sem = refs[-1]
    copies = [pltpu.make_async_copy(refs[i], refs[n + i], sem.at[i]) for i in range(n)]
    for cp in copies:
        cp.start()
    for cp in copies:
        cp.wait()


def solution(mesh):
    ep_n = mesh.shape['ep']
    tok_spec = P(('fsdp', 'ep'), None)
    row_spec = P('ep', 'fsdp', None)

    def local_backward(grad_out, expert_idx, slot_pos, gates, x_disp, h_gate, h_up, y_disp, w_gate, w_down, w_up):
        tok_n, top = expert_idx.shape
        _, rows, width = x_disp.shape
        hidden = h_gate.shape[2]
        cap = rows // ep_n
        plane = ep_n // PLANES
        ysz = 4 if plane == 16 else 2
        xsz = plane // ysz
        lanes = plane * cap
        half_d, half_f = width // 2, hidden // 2
        cfg = (ep_n, top, tok_n, width, hidden, cap, ysz, xsz)
        vmem = pl.BlockSpec(memory_space=pltpu.VMEM)
        hbm = pl.BlockSpec(memory_space=pltpu.HBM)
        dma = pltpu.SemaphoreType.DMA
        rows_buf = pltpu.VMEM((ep_n, cap, width), BF16)
        line_buf = pltpu.VMEM((PLANES, 1, lanes), F32)
        gate_buf = pltpu.VMEM((plane, PLANES, 1, lanes), F32)
        in_part = pltpu.VMEM((half_d, hidden), F32)
        out_part = pltpu.VMEM((half_f, width), F32)
        results = [
            jax.ShapeDtypeStruct((tok_n, width), BF16),
            jax.ShapeDtypeStruct((top, tok_n), F32),
            jax.ShapeDtypeStruct((half_d, hidden), F32),
            jax.ShapeDtypeStruct((half_f, width), F32),
            jax.ShapeDtypeStruct((half_d, hidden), F32),
        ]
        outs = pl.pallas_call(
            functools.partial(layer_kernel, cfg),
            out_shape=results,
            in_specs=[hbm] * 11,
            out_specs=[vmem] * 5,
            scratch_shapes=[
                pltpu.VMEM((tok_n, width), BF16), pltpu.VMEM((top, tok_n), jnp.int32), pltpu.VMEM((top, tok_n), jnp.int32),
                pltpu.VMEM((top, tok_n), F32), rows_buf, rows_buf, line_buf, line_buf, gate_buf, rows_buf, rows_buf, gate_buf, gate_buf, line_buf, line_buf,
                rows_buf, rows_buf, pltpu.VMEM((ep_n, cap, hidden), BF16), pltpu.VMEM((ep_n, cap, hidden), BF16),
                pltpu.VMEM((width, 2 * hidden), BF16), pltpu.VMEM((hidden, width), BF16),
                pltpu.VMEM((PLANES, lanes, tok_n), BF16),
                pltpu.VMEM((rows, width), BF16), pltpu.VMEM((rows, hidden), BF16), pltpu.VMEM((rows, 2 * hidden), BF16),
                in_part, out_part, in_part, in_part, out_part, in_part,
                dma((11,)), dma((3,)), dma((3,)), dma, dma((PLANES,)), dma((2,)), dma((2,)),
                dma, dma((PLANES,)), dma((2,)), dma((2,)), dma((3,)), dma((3,)),
            ],
            compiler_params=pltpu.CompilerParams(collective_id=0, has_side_effects=True, vmem_limit_bytes=44 * 1024 * 1024),
            name='layer',
        )(*[pltpu.with_memory_space_constraint(v, pltpu.HBM) for v in (grad_out, expert_idx.T, slot_pos.T, gates.T, *[v.reshape(ep_n, cap, v.shape[2]) for v in (x_disp, h_gate, h_up, y_disp)], w_gate[0], w_down[0], w_up[0])])
        gx, gg, dwg, dwd, dwu = pl.pallas_call(
            write_kernel,
            out_shape=results,
            in_specs=[vmem] * 5,
            out_specs=[hbm] * 5,
            scratch_shapes=[dma((5,))],
            compiler_params=pltpu.CompilerParams(vmem_limit_bytes=8 * 1024 * 1024),
            name='write',
        )(*outs)
        return gx, gg.T, dwg[None], dwd[None], dwu[None]

    return jax.shard_map(local_backward, mesh=mesh, in_specs=(tok_spec, tok_spec, tok_spec, tok_spec, row_spec, row_spec, row_spec, row_spec, row_spec, row_spec, row_spec), out_specs=(tok_spec, tok_spec, row_spec, row_spec, row_spec), check_vma=False)
```

```python
import functools

import jax
import jax.numpy as jnp
from jax import lax
from jax.experimental import pallas as pl
from jax.experimental.pallas import tpu as pltpu
from jax.sharding import PartitionSpec as P

MESH = pl.DeviceIdType.MESH
F32 = jnp.float32
BF16 = jnp.bfloat16
PLANES = 4
NT = (((1,), (1,)), ((), ()))
TN = (((0,), (0,)), ((), ()))


def even_chunks(ysz, xsz):
    order = [((dy + dx + k) % PLANES, dy, dx) for k in (1, 2, 3, 0) for dy in range(ysz) for dx in range(xsz)]
    return [o for o in order if o != (0, 0, 0)] + [(0, 0, 0)]


def layer_kernel(cfg, go_in, eidx_in, slot_in, gates_in, x_in, hg_in, hu_in, y_in, wg_in, wd_in, wu_in,
                 gx, gg, og, od, ou,
                 go, eidx, slot, gates, send, recv, gsend, gz, grecv, dxs, dxr, vs, vr, vsum, back4,
                 xv, yv, hgv, huv, wgu, wd, onehot, gv, av, dhv,
                 pg, pd, pu, rg, rd, ru,
                 load_sem, wsend_sem, wrecv_sem, fsend_sem, frecv_sem, gsend_sem, grecv_sem,
                 bsend_sem, brecv_sem, vsend_sem, vrecv_sem, psend_sem, precv_sem):
    ep_n, top, tok_n, width, hidden, cap, ysz, xsz = cfg
    plane = ep_n // PLANES
    lanes = plane * cap
    rows_chunk = plane * cap
    half_d, half_f = width // 2, hidden // 2
    q = lax.axis_index('fsdp')
    me = lax.axis_index('ep')
    other = 1 - q
    my_plane = me // plane
    my_in = lax.rem(me, plane)

    my_y, my_x = my_in // xsz, lax.rem(my_in, xsz)

    def walk(c, k, n):
        return lax.rem(c + (1 - 2 * lax.rem(c, 2)) * k + n, n)

    def peer_in(o):
        return walk(my_y, o // xsz, ysz) * xsz + walk(my_x, lax.rem(o, xsz), xsz)

    offsets = even_chunks(ysz, xsz)
    own = ep_n - 1

    def peer(pos):
        dz, dy, dx = offsets[pos]
        return walk(my_plane, dz, PLANES), walk(my_y, dy, ysz) * xsz + walk(my_x, dx, xsz)

    barrier = pltpu.get_barrier_semaphore()

    def announce(o, c):
        pl.semaphore_signal(barrier, inc=1, device_id=(q, lax.rem(me + o, ep_n)), device_id_type=MESH)
        return c

    lax.fori_loop(1, ep_n, announce, 0)
    pl.semaphore_signal(barrier, inc=1, device_id=(other, me), device_id_type=MESH)

    small = [
        pltpu.make_async_copy(src, dst, load_sem.at[7 + i])
        for i, (src, dst) in enumerate(((eidx_in, eidx), (slot_in, slot), (gates_in, gates), (go_in, go)))
    ]
    for cp in small:
        cp.start()
    loads = [
        pltpu.make_async_copy(wd_in, wd.at[pl.ds(q * half_f, half_f)], load_sem.at[0]),
        pltpu.make_async_copy(wg_in, wgu.at[pl.ds(q * half_d, half_d), pl.ds(0, hidden)], load_sem.at[1]),
        pltpu.make_async_copy(wu_in, wgu.at[pl.ds(q * half_d, half_d), pl.ds(hidden, hidden)], load_sem.at[2]),
    ]
    for cp in loads:
        cp.start()

    for cp in small:
        cp.wait()
    kept = slot[...] >= 0
    dest = jnp.where(kept, eidx[...] * cap + slot[...], ep_n * cap)

    def steps(place, c, n):
        return ((1 - 2 * lax.rem(c, 2)) * (place - c) + 2 * n) & (n - 1)

    place_in = eidx[...] & (plane - 1)
    dz = steps(eidx[...] >> (plane.bit_length() - 1), my_plane, PLANES)
    dy = steps(place_in >> (xsz.bit_length() - 1), my_y, ysz)
    dx = steps(place_in & (xsz - 1), my_x, xsz)
    off = (dz * ysz + dy) * xsz + dx
    pos_of = jnp.zeros_like(off)
    for pos, (kz, ky, kx) in enumerate(offsets):
        pos_of = jnp.where(off == (kz * ysz + ky) * xsz + kx, pos, pos_of)
    dest_pos = jnp.where(kept, pos_of * cap + slot[...], ep_n * cap)
    slot_s = lax.broadcasted_iota(jnp.int32, (lanes, tok_n), 0)
    diag = lax.broadcasted_iota(jnp.int32, (lanes, lanes), 0) == lax.broadcasted_iota(jnp.int32, (lanes, lanes), 1)
    for k in range(PLANES):
        hot = jnp.zeros((lanes, tok_n), F32)
        gate = jnp.zeros((lanes, tok_n), F32)
        for j in range(top):
            hot = jnp.where(slot_s == dest_pos[j:j + 1, :] - k * lanes, 1.0, hot)
            gate = jnp.where(slot_s == dest[j:j + 1, :] - k * lanes, gates[j:j + 1, :], gate)
        hot = hot.astype(BF16)
        onehot[k] = hot
        gate_col = jnp.sum(gate, axis=1, keepdims=True)
        gsend[k] = jnp.sum(jnp.where(diag, gate_col, 0.0), axis=0, keepdims=True)
        picked = jnp.dot(hot, go[...], preferred_element_type=F32)
        send[pl.ds(k * plane, plane)] = picked.reshape(plane, cap, width).astype(BF16)

    pl.semaphore_wait(barrier, ep_n)

    def partner_copy(src, dst, i, ssem, rsem):
        return pltpu.make_async_remote_copy(src_ref=src, dst_ref=dst, send_sem=ssem.at[i], recv_sem=rsem.at[i],
                                            device_id=(other, me), device_id_type=MESH)

    wcopies = [
        partner_copy(wd_in, wd.at[pl.ds(q * half_f, half_f)], 0, wsend_sem, wrecv_sem),
        partner_copy(wg_in, wgu.at[pl.ds(q * half_d, half_d), pl.ds(0, hidden)], 1, wsend_sem, wrecv_sem),
        partner_copy(wu_in, wgu.at[pl.ds(q * half_d, half_d), pl.ds(hidden, hidden)], 2, wsend_sem, wrecv_sem),
    ]
    for cp in wcopies:
        cp.start()

    def row_copy(src, dst, pos, ssem, rsem):
        zt, it = peer(pos)
        return pltpu.make_async_remote_copy(src_ref=src.at[pos], dst_ref=dst.at[pos], send_sem=ssem,
                                            recv_sem=rsem.at[pos // plane], device_id=(q, zt * plane + it), device_id_type=MESH)

    def line_copy(dz, src, dst, ssem, rsem):
        zt = lax.rem(my_plane + dz, PLANES)
        return pltpu.make_async_remote_copy(src_ref=src.at[zt], dst_ref=dst.at[my_plane], send_sem=ssem, recv_sem=rsem,
                                            device_id=(q, zt * plane + my_in), device_id_type=MESH)

    def in_plane_copy(o, src, dst, ssem, rsem):
        to = peer_in(o)
        part = src if len(src.shape) == 3 else src.at[to]
        return pltpu.make_async_remote_copy(src_ref=part, dst_ref=dst.at[my_in], send_sem=ssem, recv_sem=rsem,
                                            device_id=(q, my_plane * plane + to), device_id_type=MESH)

    def wait_bytes(buf, n, sem):
        part = buf.at[pl.ds(0, n)]
        pltpu.make_async_copy(part, part, sem).wait()

    def send_rows(lo, hi):
        for pos in range(lo, hi):
            row_copy(send, recv, pos, fsend_sem, frecv_sem).start()

    for dz in range(1, PLANES):
        line_copy(dz, gsend, gz, gsend_sem.at[0], grecv_sem.at[0]).start()
    send_rows(0, 2 * plane)
    recv[own] = send[own]
    gz[my_plane] = gsend[my_plane]
    wait_bytes(gz, PLANES - 1, grecv_sem.at[0])

    def spread(o, c):
        in_plane_copy(o, gz, grecv, gsend_sem.at[1], grecv_sem.at[1]).start()
        return c

    lax.fori_loop(1, plane, spread, 0)
    grecv[my_in] = gz[...]
    send_rows(2 * plane, own)

    for pos in range(ep_n):
        zt, it = peer(pos)
        src = zt * plane + it
        pltpu.make_async_copy(hg_in.at[src], hgv.at[pos], load_sem.at[3]).start()
        pltpu.make_async_copy(hu_in.at[src], huv.at[pos], load_sem.at[4]).start()
        pltpu.make_async_copy(y_in.at[src], yv.at[pos], load_sem.at[5]).start()
        pltpu.make_async_copy(x_in.at[src], xv.at[pos], load_sem.at[6]).start()

    def in_chunk(ci):
        return plane - 1 if ci == PLANES - 1 else plane

    for i in (0, 1, 2):
        loads[i].wait()
        wcopies[i].wait()
    wait_bytes(hgv, ep_n, load_sem.at[3])
    wait_bytes(huv, ep_n, load_sem.at[4])
    wait_bytes(yv, ep_n, load_sem.at[5])
    wait_bytes(grecv, plane - 1, grecv_sem.at[1])

    lane_c = lax.broadcasted_iota(jnp.int32, (plane, cap, lanes), 2)
    sub_c = lax.broadcasted_iota(jnp.int32, (plane, cap, lanes), 1)
    mine = lane_c == my_in * cap + sub_c

    def chunk(ci):
        wait_bytes(recv, in_chunk(ci), frecv_sem.at[ci])
        rows = pl.ds(ci * rows_chunk, rows_chunk)
        blocks = pl.ds(ci * plane, plane)
        places = [peer(ci * plane + i) for i in range(plane)]
        dy = recv[blocks].astype(F32).reshape(rows_chunk, width)
        gate3 = jnp.where(mine, jnp.broadcast_to(jnp.stack([grecv[it, zt] for zt, it in places]), (plane, cap, lanes)), 0.0)
        gate = jnp.sum(gate3, axis=2, keepdims=True).reshape(rows_chunk, 1)
        g = (dy * gate).astype(BF16)
        gv[rows] = g
        val = jnp.sum(dy * yv[blocks].astype(F32).reshape(rows_chunk, width), axis=1, keepdims=True).reshape(plane, cap, 1)
        spread_val = jnp.sum(jnp.where(mine, val, 0.0), axis=1, keepdims=True)
        for i, (zt, it) in enumerate(places):
            vs[it, zt] = spread_val[i]

        if ci == PLANES - 1:
            def gather_back(o, cc):
                in_plane_copy(o, vs, vr, vsend_sem.at[0], vrecv_sem.at[0]).start()
                return cc

            lax.fori_loop(1, plane, gather_back, 0)

        da = lax.dot_general(g, wd[...], NT, preferred_element_type=F32)
        h1 = hgv[blocks].astype(F32).reshape(rows_chunk, hidden)
        h3 = huv[blocks].astype(F32).reshape(rows_chunk, hidden)
        sg = jax.nn.sigmoid(h1)
        silu = h1 * sg
        av[rows] = jnp.where(gate > 0.0, silu * h3, 0.0).astype(BF16)
        dhv[rows, pl.ds(0, hidden)] = (da * h3 * sg * (1.0 + h1 * (1.0 - sg))).astype(BF16)
        dhv[rows, pl.ds(hidden, hidden)] = (da * silu).astype(BF16)
        dx = lax.dot_general(dhv[rows], wgu[...], NT, preferred_element_type=F32)
        dxs[blocks] = dx.reshape(plane, cap, width).astype(BF16)

        for i in range(in_chunk(ci)):
            row_copy(dxs, dxr, ci * plane + i, bsend_sem, brecv_sem).start()

    for ci in range(PLANES):
        chunk(ci)
    dxr[own] = dxs[own]
    vr[my_in] = vs[my_in]

    wait_bytes(xv, ep_n, load_sem.at[6])

    def in_grads(base, to_g, to_u):
        tile = 256 if half_d % 256 == 0 else half_d

        def step(i, c):
            cols = pl.ds(pl.multiple_of(base + i * tile, tile), tile)
            xt = xv[:, :, cols].astype(F32).reshape(ep_n * cap, tile).astype(BF16)
            r = lax.dot_general(xt, dhv[...], TN, preferred_element_type=F32)
            to_g[pl.ds(i * tile, tile)] = r[:, :hidden]
            to_u[pl.ds(i * tile, tile)] = r[:, hidden:]
            return c

        lax.fori_loop(0, half_d // tile, step, 0)

    def out_grads(base, to_d):
        cols = pl.ds(pl.multiple_of(base, half_f), half_f)
        to_d[...] = lax.dot_general(av[:, cols], gv[...], TN, preferred_element_type=F32)

    in_grads(other * half_d, pg, pu)
    pcopies = [partner_copy(pg, rg, 0, psend_sem, precv_sem), partner_copy(pu, ru, 1, psend_sem, precv_sem)]
    pcopies[0].start()
    pcopies[1].start()
    out_grads(other * half_f, pd)
    pcopies.append(partner_copy(pd, rd, 2, psend_sem, precv_sem))
    pcopies[2].start()
    in_grads(q * half_d, og, ou)
    wait_bytes(vr, plane - 1, vrecv_sem.at[0])
    total = jnp.sum(vr[...], axis=0)
    vsum[...] = total
    back4[my_plane] = vsum[my_plane]
    out_grads(q * half_f, od)
    for dz in range(1, PLANES):
        line_copy(dz, vsum, back4, vsend_sem.at[1], vrecv_sem.at[1]).start()
    for i, (mine_ref, got) in enumerate(((og, rg), (ou, ru), (od, rd))):
        pcopies[i].wait()
        mine_ref[...] += got[...]

    wait_bytes(back4, PLANES - 1, vrecv_sem.at[1])
    acc = jnp.zeros((tok_n, width), F32)
    vals = [jnp.zeros((lanes, tok_n), F32) for _ in range(top)]
    for zp in range(PLANES):
        wait_bytes(dxr, in_chunk(zp), brecv_sem.at[zp])
        blocks = pl.ds(zp * plane, plane)
        part = dxr[blocks].astype(F32).reshape(rows_chunk, width).astype(BF16)
        acc = acc + lax.dot_general(onehot[zp], part, TN, preferred_element_type=F32)
        back = jnp.sum(jnp.where(diag, back4[zp], 0.0), axis=1, keepdims=True)
        for j in range(top):
            hit = slot_s == dest[j:j + 1, :] - zp * lanes
            vals[j] = jnp.where(hit, back, vals[j])
    gx[...] = acc.astype(BF16)
    for j in range(top):
        gg[j:j + 1, :] = jnp.sum(vals[j], axis=0, keepdims=True)

    wait_bytes(send, ep_n - 1, fsend_sem)
    wait_bytes(gz, PLANES - 1, gsend_sem.at[0])
    wait_bytes(grecv, plane - 1, gsend_sem.at[1])
    wait_bytes(dxs, ep_n - 1, bsend_sem)
    wait_bytes(vr, plane - 1, vsend_sem.at[0])
    wait_bytes(back4, PLANES - 1, vsend_sem.at[1])


def write_kernel(*refs):
    n = len(refs) // 2
    sem = refs[-1]
    copies = [pltpu.make_async_copy(refs[i], refs[n + i], sem.at[i]) for i in range(n)]
    for cp in copies:
        cp.start()
    for cp in copies:
        cp.wait()


def solution(mesh):
    ep_n = mesh.shape['ep']
    tok_spec = P(('fsdp', 'ep'), None)
    row_spec = P('ep', 'fsdp', None)

    def local_backward(grad_out, expert_idx, slot_pos, gates, x_disp, h_gate, h_up, y_disp, w_gate, w_down, w_up):
        tok_n, top = expert_idx.shape
        _, rows, width = x_disp.shape
        hidden = h_gate.shape[2]
        cap = rows // ep_n
        plane = ep_n // PLANES
        ysz = 4 if plane == 16 else 2
        xsz = plane // ysz
        lanes = plane * cap
        half_d, half_f = width // 2, hidden // 2
        cfg = (ep_n, top, tok_n, width, hidden, cap, ysz, xsz)
        vmem = pl.BlockSpec(memory_space=pltpu.VMEM)
        hbm = pl.BlockSpec(memory_space=pltpu.HBM)
        dma = pltpu.SemaphoreType.DMA
        rows_buf = pltpu.VMEM((ep_n, cap, width), BF16)
        line_buf = pltpu.VMEM((PLANES, 1, lanes), F32)
        gate_buf = pltpu.VMEM((plane, PLANES, 1, lanes), F32)
        in_part = pltpu.VMEM((half_d, hidden), F32)
        out_part = pltpu.VMEM((half_f, width), F32)
        results = [
            jax.ShapeDtypeStruct((tok_n, width), BF16),
            jax.ShapeDtypeStruct((top, tok_n), F32),
            jax.ShapeDtypeStruct((half_d, hidden), F32),
            jax.ShapeDtypeStruct((half_f, width), F32),
            jax.ShapeDtypeStruct((half_d, hidden), F32),
        ]
        outs = pl.pallas_call(
            functools.partial(layer_kernel, cfg),
            out_shape=results,
            in_specs=[hbm] * 11,
            out_specs=[vmem] * 5,
            scratch_shapes=[
                pltpu.VMEM((tok_n, width), BF16), pltpu.VMEM((top, tok_n), jnp.int32), pltpu.VMEM((top, tok_n), jnp.int32),
                pltpu.VMEM((top, tok_n), F32), rows_buf, rows_buf, line_buf, line_buf, gate_buf, rows_buf, rows_buf, gate_buf, gate_buf, line_buf, line_buf,
                rows_buf, rows_buf, pltpu.VMEM((ep_n, cap, hidden), BF16), pltpu.VMEM((ep_n, cap, hidden), BF16),
                pltpu.VMEM((width, 2 * hidden), BF16), pltpu.VMEM((hidden, width), BF16),
                pltpu.VMEM((PLANES, lanes, tok_n), BF16),
                pltpu.VMEM((rows, width), BF16), pltpu.VMEM((rows, hidden), BF16), pltpu.VMEM((rows, 2 * hidden), BF16),
                in_part, out_part, in_part, in_part, out_part, in_part,
                dma((11,)), dma((3,)), dma((3,)), dma, dma((PLANES,)), dma((2,)), dma((2,)),
                dma, dma((PLANES,)), dma((2,)), dma((2,)), dma((3,)), dma((3,)),
            ],
            compiler_params=pltpu.CompilerParams(collective_id=0, has_side_effects=True, vmem_limit_bytes=44 * 1024 * 1024),
            name='layer',
        )(*[pltpu.with_memory_space_constraint(v, pltpu.HBM) for v in (grad_out, expert_idx.T, slot_pos.T, gates.T, *[v.reshape(ep_n, cap, v.shape[2]) for v in (x_disp, h_gate, h_up, y_disp)], w_gate[0], w_down[0], w_up[0])])
        gx, gg, dwg, dwd, dwu = pl.pallas_call(
            write_kernel,
            out_shape=results,
            in_specs=[vmem] * 5,
            out_specs=[hbm] * 5,
            scratch_shapes=[dma((5,))],
            compiler_params=pltpu.CompilerParams(vmem_limit_bytes=8 * 1024 * 1024),
            name='write',
        )(*outs)
        return gx, gg.T, dwg[None], dwd[None], dwu[None]

    return jax.shard_map(local_backward, mesh=mesh, in_specs=(tok_spec, tok_spec, tok_spec, tok_spec, row_spec, row_spec, row_spec, row_spec, row_spec, row_spec, row_spec), out_specs=(tok_spec, tok_spec, row_spec, row_spec, row_spec), check_vma=False)
```

```python
import functools

import jax
import jax.numpy as jnp
from jax import lax
from jax.experimental import pallas as pl
from jax.experimental.pallas import tpu as pltpu
from jax.sharding import PartitionSpec as P

MESH = pl.DeviceIdType.MESH
F32 = jnp.float32
BF16 = jnp.bfloat16
PLANES = 4
WRITE_PARTS = 4
NT = (((1,), (1,)), ((), ()))
TN = (((0,), (0,)), ((), ()))


def even_chunks(ysz, xsz):
    order = [((dy + dx + k) % PLANES, dy, dx) for k in (1, 2, 3, 0) for dy in range(ysz) for dx in range(xsz)]
    return [o for o in order if o != (0, 0, 0)] + [(0, 0, 0)]


def layer_kernel(cfg, go_in, eidx_in, slot_in, gates_in, x_in, hg_in, hu_in, y_in, wg_in, wd_in, wu_in,
                 gx, gg, og, od, ou,
                 go, eidx, slot, gates, send, recv, gsend, gz, grecv, dxs, dxr, vs, vr, vsum, back4,
                 xv, yv, hgv, huv, wgu, wd, onehot, gv, av, dhv,
                 pg, pd, pu, rg, rd, ru,
                 load_sem, wsend_sem, wrecv_sem, fsend_sem, frecv_sem, gsend_sem, grecv_sem,
                 bsend_sem, brecv_sem, vsend_sem, vrecv_sem, psend_sem, precv_sem):
    ep_n, top, tok_n, width, hidden, cap, ysz, xsz = cfg
    plane = ep_n // PLANES
    lanes = plane * cap
    rows_chunk = plane * cap
    half_d, half_f = width // 2, hidden // 2
    q = lax.axis_index('fsdp')
    me = lax.axis_index('ep')
    other = 1 - q
    my_plane = me // plane
    my_in = lax.rem(me, plane)

    my_y, my_x = my_in // xsz, lax.rem(my_in, xsz)

    def walk(c, k, n):
        return lax.rem(c + (1 - 2 * lax.rem(c, 2)) * k + n, n)

    def peer_in(o):
        return walk(my_y, o // xsz, ysz) * xsz + walk(my_x, lax.rem(o, xsz), xsz)

    offsets = even_chunks(ysz, xsz)
    own = ep_n - 1

    def peer(pos):
        dz, dy, dx = offsets[pos]
        return walk(my_plane, dz, PLANES), walk(my_y, dy, ysz) * xsz + walk(my_x, dx, xsz)

    barrier = pltpu.get_barrier_semaphore()

    def hops(pos):
        return sum(min(k, n - k) for k, n in zip(offsets[pos], (PLANES, ysz, xsz)))

    for pos in sorted(range(own), key=lambda p: -hops(p)):
        zt, it = peer(pos)
        pl.semaphore_signal(barrier, inc=1, device_id=(q, zt * plane + it), device_id_type=MESH)
    pl.semaphore_signal(barrier, inc=1, device_id=(other, me), device_id_type=MESH)

    small = [
        pltpu.make_async_copy(src, dst, load_sem.at[7 + i])
        for i, (src, dst) in enumerate(((eidx_in, eidx), (slot_in, slot), (gates_in, gates), (go_in, go)))
    ]
    for cp in small:
        cp.start()
    loads = [
        pltpu.make_async_copy(wd_in, wd.at[pl.ds(q * half_f, half_f)], load_sem.at[0]),
        pltpu.make_async_copy(wg_in, wgu.at[pl.ds(q * half_d, half_d), pl.ds(0, hidden)], load_sem.at[1]),
        pltpu.make_async_copy(wu_in, wgu.at[pl.ds(q * half_d, half_d), pl.ds(hidden, hidden)], load_sem.at[2]),
    ]
    for cp in loads:
        cp.start()

    for cp in small:
        cp.wait()
    kept = slot[...] >= 0
    dest = jnp.where(kept, eidx[...] * cap + slot[...], ep_n * cap)

    def steps(place, c, n):
        return ((1 - 2 * lax.rem(c, 2)) * (place - c) + 2 * n) & (n - 1)

    place_in = eidx[...] & (plane - 1)
    dz = steps(eidx[...] >> (plane.bit_length() - 1), my_plane, PLANES)
    dy = steps(place_in >> (xsz.bit_length() - 1), my_y, ysz)
    dx = steps(place_in & (xsz - 1), my_x, xsz)
    off = (dz * ysz + dy) * xsz + dx
    pos_of = jnp.zeros_like(off)
    for pos, (kz, ky, kx) in enumerate(offsets):
        pos_of = jnp.where(off == (kz * ysz + ky) * xsz + kx, pos, pos_of)
    dest_pos = jnp.where(kept, pos_of * cap + slot[...], ep_n * cap)
    slot_s = lax.broadcasted_iota(jnp.int32, (lanes, tok_n), 0)
    diag = lax.broadcasted_iota(jnp.int32, (lanes, lanes), 0) == lax.broadcasted_iota(jnp.int32, (lanes, lanes), 1)
    for k in range(PLANES):
        hot = jnp.zeros((lanes, tok_n), F32)
        gate = jnp.zeros((lanes, tok_n), F32)
        for j in range(top):
            hot = jnp.where(slot_s == dest_pos[j:j + 1, :] - k * lanes, 1.0, hot)
            gate = jnp.where(slot_s == dest[j:j + 1, :] - k * lanes, gates[j:j + 1, :], gate)
        hot = hot.astype(BF16)
        onehot[k] = hot
        gate_col = jnp.sum(gate, axis=1, keepdims=True)
        gsend[k] = jnp.sum(jnp.where(diag, gate_col, 0.0), axis=0, keepdims=True)
        picked = jnp.dot(hot, go[...], preferred_element_type=F32)
        send[pl.ds(k * plane, plane)] = picked.reshape(plane, cap, width).astype(BF16)

    pl.semaphore_wait(barrier, ep_n)

    def partner_copy(src, dst, i, ssem, rsem):
        return pltpu.make_async_remote_copy(src_ref=src, dst_ref=dst, send_sem=ssem.at[i], recv_sem=rsem.at[i],
                                            device_id=(other, me), device_id_type=MESH)

    wcopies = [
        partner_copy(wd_in, wd.at[pl.ds(q * half_f, half_f)], 0, wsend_sem, wrecv_sem),
        partner_copy(wg_in, wgu.at[pl.ds(q * half_d, half_d), pl.ds(0, hidden)], 1, wsend_sem, wrecv_sem),
        partner_copy(wu_in, wgu.at[pl.ds(q * half_d, half_d), pl.ds(hidden, hidden)], 2, wsend_sem, wrecv_sem),
    ]
    for cp in wcopies:
        cp.start()

    def row_copy(src, dst, pos, ssem, rsem):
        zt, it = peer(pos)
        return pltpu.make_async_remote_copy(src_ref=src.at[pos], dst_ref=dst.at[pos], send_sem=ssem,
                                            recv_sem=rsem.at[pos // plane], device_id=(q, zt * plane + it), device_id_type=MESH)

    def line_copy(dz, src, dst, ssem, rsem):
        zt = lax.rem(my_plane + dz, PLANES)
        return pltpu.make_async_remote_copy(src_ref=src.at[zt], dst_ref=dst.at[my_plane], send_sem=ssem, recv_sem=rsem,
                                            device_id=(q, zt * plane + my_in), device_id_type=MESH)

    def in_plane_copy(o, src, dst, ssem, rsem):
        to = peer_in(o)
        part = src if len(src.shape) == 3 else src.at[to]
        return pltpu.make_async_remote_copy(src_ref=part, dst_ref=dst.at[my_in], send_sem=ssem, recv_sem=rsem,
                                            device_id=(q, my_plane * plane + to), device_id_type=MESH)

    def wait_bytes(buf, n, sem):
        part = buf.at[pl.ds(0, n)]
        pltpu.make_async_copy(part, part, sem).wait()

    def send_rows(lo, hi):
        for pos in range(lo, hi):
            row_copy(send, recv, pos, fsend_sem, frecv_sem).start()

    for dz in range(1, PLANES):
        line_copy(dz, gsend, gz, gsend_sem.at[0], grecv_sem.at[0]).start()
    send_rows(0, 2 * plane)
    recv[own] = send[own]
    gz[my_plane] = gsend[my_plane]
    wait_bytes(gz, PLANES - 1, grecv_sem.at[0])

    def spread(o, c):
        in_plane_copy(o, gz, grecv, gsend_sem.at[1], grecv_sem.at[1]).start()
        return c

    lax.fori_loop(1, plane, spread, 0)
    grecv[my_in] = gz[...]
    send_rows(2 * plane, own)

    for pos in range(ep_n):
        zt, it = peer(pos)
        src = zt * plane + it
        pltpu.make_async_copy(hg_in.at[src], hgv.at[pos], load_sem.at[3]).start()
        pltpu.make_async_copy(hu_in.at[src], huv.at[pos], load_sem.at[4]).start()
        pltpu.make_async_copy(y_in.at[src], yv.at[pos], load_sem.at[5]).start()
        pltpu.make_async_copy(x_in.at[src], xv.at[pos], load_sem.at[6]).start()

    def in_chunk(ci):
        return plane - 1 if ci == PLANES - 1 else plane

    for i in (0, 1, 2):
        loads[i].wait()
        wcopies[i].wait()
    wait_bytes(hgv, ep_n, load_sem.at[3])
    wait_bytes(huv, ep_n, load_sem.at[4])
    wait_bytes(yv, ep_n, load_sem.at[5])
    wait_bytes(grecv, plane - 1, grecv_sem.at[1])

    lane_c = lax.broadcasted_iota(jnp.int32, (plane, cap, lanes), 2)
    sub_c = lax.broadcasted_iota(jnp.int32, (plane, cap, lanes), 1)
    mine = lane_c == my_in * cap + sub_c

    def chunk(ci):
        wait_bytes(recv, in_chunk(ci), frecv_sem.at[ci])
        rows = pl.ds(ci * rows_chunk, rows_chunk)
        blocks = pl.ds(ci * plane, plane)
        places = [peer(ci * plane + i) for i in range(plane)]
        dy = recv[blocks].astype(F32).reshape(rows_chunk, width)
        gate3 = jnp.where(mine, jnp.broadcast_to(jnp.stack([grecv[it, zt] for zt, it in places]), (plane, cap, lanes)), 0.0)
        gate = jnp.sum(gate3, axis=2, keepdims=True).reshape(rows_chunk, 1)
        g = (dy * gate).astype(BF16)
        gv[rows] = g
        val = jnp.sum(dy * yv[blocks].astype(F32).reshape(rows_chunk, width), axis=1, keepdims=True).reshape(plane, cap, 1)
        spread_val = jnp.sum(jnp.where(mine, val, 0.0), axis=1, keepdims=True)
        for i, (zt, it) in enumerate(places):
            vs[it, zt] = spread_val[i]

        if ci == PLANES - 1:
            def gather_back(o, cc):
                in_plane_copy(o, vs, vr, vsend_sem.at[0], vrecv_sem.at[0]).start()
                return cc

            lax.fori_loop(1, plane, gather_back, 0)

        da = lax.dot_general(g, wd[...], NT, preferred_element_type=F32)
        h1 = hgv[blocks].astype(F32).reshape(rows_chunk, hidden)
        h3 = huv[blocks].astype(F32).reshape(rows_chunk, hidden)
        sg = jax.nn.sigmoid(h1)
        silu = h1 * sg
        av[rows] = jnp.where(gate > 0.0, silu * h3, 0.0).astype(BF16)
        dhv[rows, pl.ds(0, hidden)] = (da * h3 * sg * (1.0 + h1 * (1.0 - sg))).astype(BF16)
        dhv[rows, pl.ds(hidden, hidden)] = (da * silu).astype(BF16)
        dx = lax.dot_general(dhv[rows], wgu[...], NT, preferred_element_type=F32)
        dxs[blocks] = dx.reshape(plane, cap, width).astype(BF16)

        for i in range(in_chunk(ci)):
            row_copy(dxs, dxr, ci * plane + i, bsend_sem, brecv_sem).start()

    for ci in range(PLANES):
        chunk(ci)
    dxr[own] = dxs[own]
    vr[my_in] = vs[my_in]

    wait_bytes(xv, ep_n, load_sem.at[6])

    def in_grads(base, to_g, to_u):
        tile = 256 if half_d % 256 == 0 else half_d

        def step(i, c):
            cols = pl.ds(pl.multiple_of(base + i * tile, tile), tile)
            xt = xv[:, :, cols].astype(F32).reshape(ep_n * cap, tile).astype(BF16)
            r = lax.dot_general(xt, dhv[...], TN, preferred_element_type=F32)
            to_g[pl.ds(i * tile, tile)] = r[:, :hidden]
            to_u[pl.ds(i * tile, tile)] = r[:, hidden:]
            return c

        lax.fori_loop(0, half_d // tile, step, 0)

    def out_grads(base, to_d):
        cols = pl.ds(pl.multiple_of(base, half_f), half_f)
        to_d[...] = lax.dot_general(av[:, cols], gv[...], TN, preferred_element_type=F32)

    in_grads(other * half_d, pg, pu)
    pcopies = [partner_copy(pg, rg, 0, psend_sem, precv_sem), partner_copy(pu, ru, 1, psend_sem, precv_sem)]
    pcopies[0].start()
    pcopies[1].start()
    out_grads(other * half_f, pd)
    pcopies.append(partner_copy(pd, rd, 2, psend_sem, precv_sem))
    pcopies[2].start()
    in_grads(q * half_d, og, ou)
    wait_bytes(vr, plane - 1, vrecv_sem.at[0])
    total = jnp.sum(vr[...], axis=0)
    vsum[...] = total
    back4[my_plane] = vsum[my_plane]
    out_grads(q * half_f, od)
    for dz in range(1, PLANES):
        line_copy(dz, vsum, back4, vsend_sem.at[1], vrecv_sem.at[1]).start()
    for i, (mine_ref, got) in enumerate(((og, rg), (ou, ru), (od, rd))):
        pcopies[i].wait()
        mine_ref[...] += got[...]

    wait_bytes(back4, PLANES - 1, vrecv_sem.at[1])
    vals = [jnp.zeros((lanes, tok_n), F32) for _ in range(top)]
    for zp in range(PLANES):
        back = jnp.sum(jnp.where(diag, back4[zp], 0.0), axis=1, keepdims=True)
        for j in range(top):
            hit = slot_s == dest[j:j + 1, :] - zp * lanes
            vals[j] = jnp.where(hit, back, vals[j])
    for j in range(top):
        gg[j:j + 1, :] = jnp.sum(vals[j], axis=0, keepdims=True)
    acc = jnp.zeros((tok_n, width), F32)
    for zp in range(PLANES):
        wait_bytes(dxr, in_chunk(zp), brecv_sem.at[zp])
        blocks = pl.ds(zp * plane, plane)
        part = dxr[blocks].astype(F32).reshape(rows_chunk, width).astype(BF16)
        acc = acc + lax.dot_general(onehot[zp], part, TN, preferred_element_type=F32)
    gx[...] = acc.astype(BF16)

    wait_bytes(send, ep_n - 1, fsend_sem)
    wait_bytes(gz, PLANES - 1, gsend_sem.at[0])
    wait_bytes(grecv, plane - 1, gsend_sem.at[1])
    wait_bytes(dxs, ep_n - 1, bsend_sem)
    wait_bytes(vr, plane - 1, vsend_sem.at[0])
    wait_bytes(back4, PLANES - 1, vsend_sem.at[1])


def write_kernel(*refs):
    n = len(refs) // 2
    sem = refs[-1]
    copies = []
    for i in range(n):
        rows = refs[i].shape[0]
        parts = WRITE_PARTS if rows % (8 * WRITE_PARTS) == 0 else 1
        for p in range(parts):
            part = pl.ds(p * (rows // parts), rows // parts)
            copies.append(pltpu.make_async_copy(refs[i].at[part], refs[n + i].at[part], sem.at[i, p]))
    for cp in copies:
        cp.start()
    for cp in copies:
        cp.wait()


def solution(mesh):
    ep_n = mesh.shape['ep']
    tok_spec = P(('fsdp', 'ep'), None)
    row_spec = P('ep', 'fsdp', None)

    def local_backward(grad_out, expert_idx, slot_pos, gates, x_disp, h_gate, h_up, y_disp, w_gate, w_down, w_up):
        tok_n, top = expert_idx.shape
        _, rows, width = x_disp.shape
        hidden = h_gate.shape[2]
        cap = rows // ep_n
        plane = ep_n // PLANES
        ysz = 4 if plane == 16 else 2
        xsz = plane // ysz
        lanes = plane * cap
        half_d, half_f = width // 2, hidden // 2
        cfg = (ep_n, top, tok_n, width, hidden, cap, ysz, xsz)
        vmem = pl.BlockSpec(memory_space=pltpu.VMEM)
        hbm = pl.BlockSpec(memory_space=pltpu.HBM)
        dma = pltpu.SemaphoreType.DMA
        rows_buf = pltpu.VMEM((ep_n, cap, width), BF16)
        line_buf = pltpu.VMEM((PLANES, 1, lanes), F32)
        gate_buf = pltpu.VMEM((plane, PLANES, 1, lanes), F32)
        in_part = pltpu.VMEM((half_d, hidden), F32)
        out_part = pltpu.VMEM((half_f, width), F32)
        results = [
            jax.ShapeDtypeStruct((tok_n, width), BF16),
            jax.ShapeDtypeStruct((top, tok_n), F32),
            jax.ShapeDtypeStruct((half_d, hidden), F32),
            jax.ShapeDtypeStruct((half_f, width), F32),
            jax.ShapeDtypeStruct((half_d, hidden), F32),
        ]
        outs = pl.pallas_call(
            functools.partial(layer_kernel, cfg),
            out_shape=results,
            in_specs=[hbm] * 11,
            out_specs=[vmem] * 5,
            scratch_shapes=[
                pltpu.VMEM((tok_n, width), BF16), pltpu.VMEM((top, tok_n), jnp.int32), pltpu.VMEM((top, tok_n), jnp.int32),
                pltpu.VMEM((top, tok_n), F32), rows_buf, rows_buf, line_buf, line_buf, gate_buf, rows_buf, rows_buf, gate_buf, gate_buf, line_buf, line_buf,
                rows_buf, rows_buf, pltpu.VMEM((ep_n, cap, hidden), BF16), pltpu.VMEM((ep_n, cap, hidden), BF16),
                pltpu.VMEM((width, 2 * hidden), BF16), pltpu.VMEM((hidden, width), BF16),
                pltpu.VMEM((PLANES, lanes, tok_n), BF16),
                pltpu.VMEM((rows, width), BF16), pltpu.VMEM((rows, hidden), BF16), pltpu.VMEM((rows, 2 * hidden), BF16),
                in_part, out_part, in_part, in_part, out_part, in_part,
                dma((11,)), dma((3,)), dma((3,)), dma, dma((PLANES,)), dma((2,)), dma((2,)),
                dma, dma((PLANES,)), dma((2,)), dma((2,)), dma((3,)), dma((3,)),
            ],
            compiler_params=pltpu.CompilerParams(collective_id=0, has_side_effects=True, vmem_limit_bytes=44 * 1024 * 1024),
            name='layer',
        )(*[pltpu.with_memory_space_constraint(v, pltpu.HBM) for v in (grad_out, expert_idx.T, slot_pos.T, gates.T, *[v.reshape(ep_n, cap, v.shape[2]) for v in (x_disp, h_gate, h_up, y_disp)], w_gate[0], w_down[0], w_up[0])])
        gx, gg, dwg, dwd, dwu = pl.pallas_call(
            write_kernel,
            out_shape=results,
            in_specs=[vmem] * 5,
            out_specs=[hbm] * 5,
            scratch_shapes=[dma((5, WRITE_PARTS))],
            compiler_params=pltpu.CompilerParams(vmem_limit_bytes=8 * 1024 * 1024),
            name='write',
        )(*outs)
        return gx, gg.T, dwg[None], dwd[None], dwu[None]

    return jax.shard_map(local_backward, mesh=mesh, in_specs=(tok_spec, tok_spec, tok_spec, tok_spec, row_spec, row_spec, row_spec, row_spec, row_spec, row_spec, row_spec), out_specs=(tok_spec, tok_spec, row_spec, row_spec, row_spec), check_vma=False)
```
